8 devices in a mesh: dp: 1 (over z), tp: 2 (over y), ep: 4 (over x, core).
Axes of the slice: x: 2, y: 2, z: 1, core: 2. Of those that a mesh axis runs over, the one named last changes fastest.
Arguments:
- hidden: bfloat16 [256, 2048], P(('dp', 'ep'))
- expert_ids: int32 [256, 8], P(('dp', 'ep'))
- norm_w: bfloat16 [2048], replicated
- router_w: bfloat16 [2048, 128], replicated
- w_gate: bfloat16 [128, 2048, 768], P('ep', None, 'tp')
- w_up: bfloat16 [128, 2048, 768], P('ep', None, 'tp')
- w_down: bfloat16 [128, 768, 2048], P('ep', 'tp')
Outputs:
- output: bfloat16 [256, 2048], P(('dp', 'ep'))
All inputs are finite; a program needn't handle non-finite values.
Results may differ from the reference program's by a relative error of at most 0.00964266.
Values are sent between devices in bfloat16 or wider.
A program may use at most 1 GiB of HBM per device.

```python
import jax
import jax.numpy as jnp
from jax import lax

D = 2048
FF = 768
EXPERTS = 128
TOP = 8
TOK_DEV = 64
EP = 4
CAP = 8
TOKENS = TOK_DEV * EP
NORM_EPS = 1e-6


def random_order(order_key, count):
    order_score = jax.random.randint(order_key, (count,), 0, count) * count + jnp.arange(count, dtype=jnp.int32)
    return jnp.argsort(order_score)


def draw_routes(route_key):
    pair_count = TOP * TOK_DEV
    weight_total = (EXPERTS - 1) * (5 * EXPERTS - 2) // 2
    bounds = [CAP + ((pair_count - CAP) * (4 * rank_step * (EXPERTS - 1) - 3 * rank_step * (rank_step - 1) // 2)) // weight_total for rank_step in range(EXPERTS - 1)]
    bound_arr = jnp.array(bounds, dtype=jnp.int32)
    positions = jnp.arange(TOK_DEV, dtype=jnp.int32)[:, None] + TOK_DEV * jnp.arange(TOP, dtype=jnp.int32)[None, :]
    rank_of = jnp.sum((positions[:, :, None] >= bound_arr).astype(jnp.int32), axis=-1)
    label_key, rows_key = jax.random.split(route_key)
    labels = random_order(label_key, EXPERTS).astype(jnp.int32)
    choices = labels[rank_of]
    row_keys = jax.random.split(rows_key, EP)
    orders = jax.vmap(lambda sub_key: random_order(sub_key, TOK_DEV))(row_keys)
    return choices[orders].reshape(TOKENS, TOP).astype(jnp.int32)


def setup_inputs(seed: int = 0, part: int = 0) -> dict:
    base_key = jax.random.key(seed)
    key_list = jax.random.split(base_key, 7)
    hidden = jax.random.normal(jax.random.fold_in(key_list[0], part), (TOKENS, D), jnp.float32)
    expert_ids = draw_routes(jax.random.fold_in(key_list[1], part))
    norm_w = 1.0 + 0.3 * jax.random.normal(key_list[2], (D,), jnp.float32)
    router_w = D ** -0.5 * jax.random.normal(key_list[3], (D, EXPERTS), jnp.float32)
    w_gate = D ** -0.5 * jax.random.normal(key_list[4], (EXPERTS, D, FF), jnp.float32)
    w_up = D ** -0.5 * jax.random.normal(key_list[5], (EXPERTS, D, FF), jnp.float32)
    down_scale = 2.0 * EXPERTS / (TOP * FF) ** 0.5
    w_down = down_scale * jax.random.normal(key_list[6], (EXPERTS, FF, D), jnp.float32)
    return {"hidden": hidden.astype(jnp.bfloat16), "expert_ids": expert_ids, "norm_w": norm_w.astype(jnp.bfloat16), "router_w": router_w.astype(jnp.bfloat16), "w_gate": w_gate.astype(jnp.bfloat16), "w_up": w_up.astype(jnp.bfloat16), "w_down": w_down.astype(jnp.bfloat16)}


def rms_norm(hidden, norm_w):
    wide_h = hidden.astype(jnp.float32)
    mean_sq = jnp.mean(wide_h * wide_h, axis=-1, keepdims=True)
    return (wide_h * lax.rsqrt(mean_sq + NORM_EPS) * norm_w.astype(jnp.float32)).astype(jnp.bfloat16)


def reference(hidden, expert_ids, norm_w, router_w, w_gate, w_up, w_down):
    normed = rms_norm(hidden, norm_w)
    logits = jnp.dot(normed, router_w, preferred_element_type=jnp.float32)
    router_prob = jax.nn.softmax(logits, axis=-1)
    gate_prob = jnp.take_along_axis(router_prob, expert_ids, axis=-1).reshape(-1)
    flat_ids = expert_ids.reshape(-1)
    pair_tok = jnp.arange(TOKENS * TOP, dtype=jnp.int32) // TOP
    row_limit = EP * CAP

    def one_expert(accum, per_expert):
        expert, gate_e, up_e, down_e = per_expert
        chosen = flat_ids == expert
        (picked,) = jnp.nonzero(chosen, size=row_limit, fill_value=0)
        row_valid = jnp.arange(row_limit) < jnp.sum(chosen.astype(jnp.int32))
        tok_rows = pair_tok[picked]
        x_rows = normed[tok_rows]
        gate_pre = jnp.dot(x_rows, gate_e, preferred_element_type=jnp.float32)
        up_pre = jnp.dot(x_rows, up_e, preferred_element_type=jnp.float32)
        act_rows = (jax.nn.silu(gate_pre) * up_pre).astype(jnp.bfloat16)
        expert_out = jnp.dot(act_rows, down_e, preferred_element_type=jnp.float32).astype(jnp.bfloat16)
        weight = jnp.where(row_valid, gate_prob[picked], 0.0)
        return accum.at[tok_rows].add(weight[:, None] * expert_out.astype(jnp.float32)), None

    moe_sum, _ = lax.scan(one_expert, jnp.zeros((TOKENS, D), jnp.float32), (jnp.arange(EXPERTS, dtype=jnp.int32), w_gate, w_up, w_down))
    return (hidden.astype(jnp.float32) + moe_sum).astype(jnp.bfloat16)
```

```python
import functools

import jax
import jax.numpy as jnp
from jax import lax
from jax.experimental import pallas as pl
from jax.experimental.pallas import tpu as pltpu
from jax.sharding import PartitionSpec as P

NORM_EPS = 1e-6
RING = 10
BLK = 256
F32 = jnp.float32
BF16 = jnp.bfloat16


def row_cap(tok_dev, top_k, n_experts):
    return 8 * ((2 * top_k * tok_dev + 8 * n_experts - 1) // (8 * n_experts))


def moe_kernel(dims, h_hbm, ids_hbm, nw_hbm, rw_hbm, wg_hbm, wu_hbm, wd_hbm, out_hbm,
               ring, wdb, hbuf, idb, nwb, rwb, vbuf, xbuf, posb, cbuf, abuf, ybuf,
               sbuf, ra, tb, rb, zb, rc, obuf,
               gsem, usem, dsem, lsem, hs_sem, hr_sem, is_sem, ir_sem,
               as_sem, ar_sem, bs_sem, br_sem, cs_sem, cr_sem, osem):
    tok, top_k, n_exp, local, ff, d, cap = dims
    n_tok = 4 * tok
    slot_rows = 4 * cap
    n_slots = local * slot_rows
    n_blk = d // BLK
    tp = lax.axis_index("tp")
    ep = lax.axis_index("ep")
    x = ep // 2
    core = ep % 2
    partner = {"ep": x * 2 + (1 - core)}
    across = {"ep": (1 - x) * 2 + core}
    other = {"tp": 1 - tp}
    MESH = pl.DeviceIdType.MESH
    q_own = core * 2 + x
    q_across = core * 2 + (1 - x)
    q_partner = (1 - core) * 2 + x
    q_diag = (1 - core) * 2 + (1 - x)

    def w_copies(e, slot):
        return (
            pltpu.make_async_copy(wg_hbm.at[e], ring.at[slot, :, pl.ds(0, ff)], gsem.at[slot]),
            pltpu.make_async_copy(wu_hbm.at[e], ring.at[slot, :, pl.ds(ff, ff)], usem.at[slot]),
        )

    parts = 4
    per = local // parts

    def d_copy(c, s, k):
        return pltpu.make_async_copy(
            wd_hbm.at[pl.ds(k * per, per), :, pl.ds(pl.multiple_of(c * BLK, BLK), BLK)],
            wdb.at[s, pl.ds(k * per, per)], dsem.at[s, k])

    own_h = pltpu.make_async_copy(h_hbm, hbuf.at[q_own], lsem.at[0])
    own_i = pltpu.make_async_copy(ids_hbm, idb.at[q_own], lsem.at[1])
    nw_c = pltpu.make_async_copy(nw_hbm, nwb, lsem.at[2])
    rw_c = pltpu.make_async_copy(rw_hbm, rwb, lsem.at[3])
    for cp in (own_h, own_i, nw_c, rw_c):
        cp.start()
    for e in range(RING):
        for cp in w_copies(e, e):
            cp.start()
    for c in range(2):
        for k in range(parts):
            d_copy(c, c, k).start()

    barrier = pltpu.get_barrier_semaphore()
    for dev in (partner, across, other):
        pl.semaphore_signal(barrier, inc=1, device_id=dev, device_id_type=MESH)
    pl.semaphore_wait(barrier, 3)

    def h_copy(src, q, dev, n):
        return pltpu.make_async_remote_copy(
            src_ref=src, dst_ref=hbuf.at[q], send_sem=hs_sem.at[n], recv_sem=hr_sem.at[n],
            device_id=dev, device_id_type=MESH)

    def i_copy(src, q, dev, n):
        return pltpu.make_async_remote_copy(
            src_ref=src, dst_ref=idb.at[q], send_sem=is_sem.at[n], recv_sem=ir_sem.at[n],
            device_id=dev, device_id_type=MESH)

    i_x = i_copy(ids_hbm, q_own, across, 0)
    i_p = i_copy(ids_hbm, q_own, partner, 1)
    h_x = h_copy(h_hbm, q_own, across, 0)
    h_p = h_copy(h_hbm, q_own, partner, 1)
    i_x.start()
    i_p.start()
    h_x.start()
    h_p.start()
    i_copy(ids_hbm, q_across, across, 0).wait_recv()
    i_r = i_copy(idb.at[q_across], q_across, partner, 2)
    i_r.start()

    own_i.wait()
    i_copy(ids_hbm, q_partner, partner, 1).wait_recv()
    i_copy(idb.at[q_diag], q_diag, partner, 2).wait_recv()
    ids_t = jnp.concatenate([idb[q] for q in range(4)], axis=1)
    exp_iota = lax.broadcasted_iota(jnp.int32, (n_exp, n_tok), 0)
    member = jnp.zeros((n_exp, n_tok), F32)
    for j in range(top_k):
        member = member + jnp.where(ids_t[j:j + 1, :] == exp_iota, 1.0, 0.0)
    row_i = lax.broadcasted_iota(jnp.int32, (n_tok, n_tok), 0)
    col_i = lax.broadcasted_iota(jnp.int32, (n_tok, n_tok), 1)
    before = jnp.where(row_i < col_i, 1.0, 0.0).astype(BF16)
    pos = jnp.dot(member.astype(BF16), before, preferred_element_type=F32)
    pos = jnp.where(member > 0.5, pos, -1.0)
    posb[...] = pos

    nw_c.wait()

    def norm_rows(q):
        wide = hbuf[q].astype(F32)
        inv = lax.rsqrt(jnp.mean(wide * wide, axis=-1, keepdims=True) + NORM_EPS)
        for k in range(d // 128):
            cols = pl.ds(k * 128, 128)
            part = hbuf[q, :, cols].astype(F32) * inv * nwb[k:k + 1, :].astype(F32)
            vbuf[pl.ds(pl.multiple_of(q * tok, tok), tok), cols] = part.astype(BF16)

    own_h.wait()
    norm_rows(q_own)
    h_copy(h_hbm, q_partner, partner, 1).wait_recv()
    norm_rows(q_partner)
    h_copy(h_hbm, q_across, across, 0).wait_recv()
    h_r = h_copy(hbuf.at[q_across], q_across, partner, 2)
    h_r.start()
    norm_rows(q_across)
    h_copy(hbuf.at[q_diag], q_diag, partner, 2).wait_recv()
    norm_rows(q_diag)

    pos_loc = posb[pl.ds(pl.multiple_of(ep * local, local), local), :]
    slot_f = lax.broadcasted_iota(jnp.int32, (slot_rows, n_tok), 0).astype(F32)
    pick = jnp.concatenate(
        [jnp.where(pos_loc[e:e + 1, :] == slot_f, 1.0, 0.0).astype(BF16) for e in range(local)], axis=0)

    def gather_cols(n, carry):
        cols = pl.ds(pl.multiple_of(n * 256, 256), 256)
        v_cols = vbuf[:, cols]
        for m in range(n_slots // 256):
            rows = jnp.dot(pick[m * 256:(m + 1) * 256], v_cols, preferred_element_type=F32)
            xbuf[m * 256:(m + 1) * 256, cols] = rows.astype(BF16)
        return carry

    lax.fori_loop(0, d // 256, gather_cols, 0)

    def gate_up(e, carry):
        slot = lax.rem(e, RING)
        rows = pl.ds(pl.multiple_of(e * slot_rows, slot_rows), slot_rows)
        for cp in w_copies(e, slot):
            cp.wait()
        pre = jnp.dot(xbuf[rows, :], ring[slot], preferred_element_type=F32)
        gate, up = pre[:, :ff], pre[:, ff:]
        abuf[rows, :] = (gate * jax.nn.sigmoid(gate) * up).astype(BF16)

        @pl.when(e + RING < local)
        def _():
            for cp in w_copies(e + RING, slot):
                cp.start()
        return carry

    lax.fori_loop(0, local, gate_up, 0)

    rw_c.wait()
    logits = jnp.dot(vbuf[...], rwb[...], preferred_element_type=F32)
    expo = jnp.exp(logits - jnp.max(logits, axis=-1, keepdims=True))
    prob = expo / jnp.sum(expo, axis=-1, keepdims=True)
    g_hi = prob.astype(BF16)
    rest = prob - g_hi.astype(F32)
    g_mid = rest.astype(BF16)
    g_lo = (rest - g_mid.astype(F32)).astype(BF16)
    pos_t = posb[...].T.astype(BF16)
    for n in range(n_slots // 256):
        lane = lax.broadcasted_iota(jnp.int32, (n_exp, 256), 1) + n * 256
        sub = lax.broadcasted_iota(jnp.int32, (n_exp, 256), 0)
        spread = jnp.where(sub == ep * local + lane // slot_rows, 1.0, 0.0).astype(BF16)
        want = (lax.broadcasted_iota(jnp.int32, (n_tok, 256), 1) % slot_rows).astype(F32)
        hit = jnp.dot(pos_t, spread, preferred_element_type=F32) == want
        for i, g in enumerate((g_hi, g_mid, g_lo)):
            wide_g = jnp.dot(g, spread, preferred_element_type=F32)
            cbuf[i, :, n * 256:(n + 1) * 256] = jnp.where(hit, wide_g, 0.0).astype(BF16)

    half = n_tok // 2

    def a_copy(c, row):
        return pltpu.make_async_remote_copy(
            src_ref=sbuf.at[c, pl.ds(pl.multiple_of(row * half, half), half)], dst_ref=ra.at[c],
            send_sem=as_sem.at[c], recv_sem=ar_sem.at[c], device_id=partner, device_id_type=MESH)

    def b_copy(c):
        return pltpu.make_async_remote_copy(
            src_ref=tb.at[c, pl.ds(pl.multiple_of((1 - x) * tok, tok), tok)], dst_ref=rb.at[c],
            send_sem=bs_sem.at[c], recv_sem=br_sem.at[c], device_id=across, device_id_type=MESH)

    def c_copy(c):
        return pltpu.make_async_remote_copy(
            src_ref=zb.at[c], dst_ref=rc.at[c],
            send_sem=cs_sem.at[c], recv_sem=cr_sem.at[c], device_id=other, device_id_type=MESH)

    def o_copy(c):
        cols = pl.ds(pl.multiple_of(c * BLK, BLK), BLK)
        return pltpu.make_async_copy(obuf.at[:, cols], out_hbm.at[:, cols], osem.at[c])

    def stage_b(c):
        a_copy(c, 1 - core).wait_recv()
        tb[c] = sbuf[c, pl.ds(pl.multiple_of(core * half, half), half), :] + ra[c]
        b_copy(c).start()

    def stage_c(c):
        b_copy(c).wait_recv()
        zb[c] = tb[c, pl.ds(pl.multiple_of(x * tok, tok), tok), :] + rb[c]
        c_copy(c).start()

    def stage_d(c):
        c_copy(c).wait_recv()
        cols = pl.ds(pl.multiple_of(c * BLK, BLK), BLK)
        obuf[:, cols] = (hbuf[q_own, :, cols].astype(F32) + (zb[c] + rc[c])).astype(BF16)
        o_copy(c).start()

    LAG_B, LAG_C, LAG_D = 1, 3, 5

    def down(c, carry):
        s = lax.rem(c, 2)
        for k in range(parts):
            d_copy(c, s, k).wait()

        def one(e, inner):
            rows = pl.ds(pl.multiple_of(e * slot_rows, slot_rows), slot_rows)
            y = jnp.dot(abuf[rows, :], wdb[s, e], preferred_element_type=F32)
            ybuf[rows, :] = y.astype(BF16)
            return inner

        lax.fori_loop(0, local, one, 0)

        @pl.when(c + 2 < n_blk)
        def _():
            for k in range(parts):
                d_copy(c + 2, s, k).start()

        y_all = ybuf[...]
        total = jnp.dot(cbuf[2], y_all, preferred_element_type=F32)
        total = total + jnp.dot(cbuf[1], y_all, preferred_element_type=F32)
        total = total + jnp.dot(cbuf[0], y_all, preferred_element_type=F32)
        sbuf[c] = total
        a_copy(c, 1 - core).start()

        @pl.when(c >= LAG_B)
        def _():
            stage_b(c - LAG_B)

        @pl.when(c >= LAG_C)
        def _():
            stage_c(c - LAG_C)

        @pl.when(c >= LAG_D)
        def _():
            stage_d(c - LAG_D)
        return carry

    lax.fori_loop(0, n_blk, down, 0)
    for c in range(n_blk - LAG_B, n_blk):
        stage_b(c)
    for c in range(n_blk - LAG_C, n_blk):
        stage_c(c)
    for c in range(n_blk - LAG_D, n_blk):
        stage_d(c)

    for cp in (i_x, i_p, i_r, h_x, h_p, h_r):
        cp.wait_send()

    def drain(c, carry):
        a_copy(c, 1 - core).wait_send()
        b_copy(c).wait_send()
        c_copy(c).wait_send()
        o_copy(c).wait()
        return carry

    lax.fori_loop(0, n_blk, drain, 0)


def solution(mesh):
    def per_device(hidden, expert_ids, norm_w, router_w, w_gate, w_up, w_down):
        tok, d = hidden.shape
        top_k = expert_ids.shape[1]
        n_exp = router_w.shape[1]
        local, _, ff = w_gate.shape
        cap = row_cap(tok, top_k, n_exp)
        dims = (tok, top_k, n_exp, local, ff, d, cap)
        n_tok = 4 * tok
        n_slots = local * 4 * cap
        n_blk = d // BLK
        any_spec = pl.BlockSpec(memory_space=pl.ANY)
        dma = pltpu.SemaphoreType.DMA
        return pl.pallas_call(
            functools.partial(moe_kernel, dims),
            out_shape=jax.ShapeDtypeStruct((tok, d), BF16),
            in_specs=[any_spec] * 7,
            out_specs=any_spec,
            scratch_shapes=[
                pltpu.VMEM((RING, d, 2 * ff), BF16),
                pltpu.VMEM((2, local, ff, BLK), BF16),
                pltpu.VMEM((4, tok, d), BF16),
                pltpu.VMEM((4, top_k, tok), jnp.int32),
                pltpu.VMEM((d // 128, 128), BF16),
                pltpu.VMEM((d, n_exp), BF16),
                pltpu.VMEM((n_tok, d), BF16),
                pltpu.VMEM((n_slots, d), BF16),
                pltpu.VMEM((n_exp, n_tok), F32),
                pltpu.VMEM((3, n_tok, n_slots), BF16),
                pltpu.VMEM((n_slots, ff), BF16),
                pltpu.VMEM((n_slots, BLK), BF16),
                pltpu.VMEM((n_blk, n_tok, BLK), F32),
                pltpu.VMEM((n_blk, n_tok // 2, BLK), F32),
                pltpu.VMEM((n_blk, n_tok // 2, BLK), F32),
                pltpu.VMEM((n_blk, tok, BLK), F32),
                pltpu.VMEM((n_blk, tok, BLK), F32),
                pltpu.VMEM((n_blk, tok, BLK), F32),
                pltpu.VMEM((tok, d), BF16),
                dma((RING,)), dma((RING,)), dma((2, 4)), dma((4,)),
                dma((3,)), dma((3,)), dma((3,)), dma((3,)),
                dma((n_blk,)), dma((n_blk,)), dma((n_blk,)), dma((n_blk,)), dma((n_blk,)), dma((n_blk,)),
                dma((n_blk,)),
            ],
            compiler_params=pltpu.CompilerParams(
                collective_id=0, has_side_effects=True, vmem_limit_bytes=67043328),
            name="moe_layer",
        )(hidden, expert_ids.T, norm_w.reshape(d // 128, 128), router_w, w_gate, w_up, w_down)

    token_spec = P(("dp", "ep"), None)
    return jax.shard_map(per_device, mesh=mesh, in_specs=(token_spec, token_spec, P(None), P(None, None), P("ep", None, "tp"), P("ep", None, "tp"), P("ep", "tp", None)), out_specs=token_spec, check_vma=False)
```

```python
import functools

import jax
import jax.numpy as jnp
from jax import lax
from jax.experimental import pallas as pl
from jax.experimental.pallas import tpu as pltpu
from jax.sharding import PartitionSpec as P

NORM_EPS = 1e-6
RING = 10
UP_UNROLL = 2
DOWN_UNROLL = 8
BLK = 256
F32 = jnp.float32
BF16 = jnp.bfloat16


def row_cap(tok_dev, top_k, n_experts):
    return 8 * ((2 * top_k * tok_dev + 8 * n_experts - 1) // (8 * n_experts))


def moe_kernel(dims, h_hbm, ids_hbm, nw_hbm, rw_hbm, wg_hbm, wu_hbm, wd_hbm, out_hbm,
               ring, wdb, hbuf, idb, nwb, rwb, vbuf, xbuf, posb, cbuf, abuf, ybuf,
               sbuf, ra, tb, rb, zb, rc, obuf,
               gsem, usem, dsem, lsem, hs_sem, hr_sem, is_sem, ir_sem,
               as_sem, ar_sem, bs_sem, br_sem, cs_sem, cr_sem, osem):
    tok, top_k, n_exp, local, ff, d, cap = dims
    n_tok = 4 * tok
    slot_rows = 4 * cap
    n_slots = local * slot_rows
    n_blk = d // BLK
    tp = lax.axis_index("tp")
    ep = lax.axis_index("ep")
    x = ep // 2
    core = ep % 2
    partner = {"ep": x * 2 + (1 - core)}
    across = {"ep": (1 - x) * 2 + core}
    other = {"tp": 1 - tp}
    MESH = pl.DeviceIdType.MESH
    q_own = core * 2 + x
    q_across = core * 2 + (1 - x)
    q_partner = (1 - core) * 2 + x
    q_diag = (1 - core) * 2 + (1 - x)

    def w_copies(e, slot):
        return (
            pltpu.make_async_copy(wg_hbm.at[e], ring.at[slot, :, pl.ds(0, ff)], gsem.at[slot]),
            pltpu.make_async_copy(wu_hbm.at[e], ring.at[slot, :, pl.ds(ff, ff)], usem.at[slot]),
        )

    parts = 4
    per = local // parts

    def d_copy(c, s, k):
        return pltpu.make_async_copy(
            wd_hbm.at[pl.ds(k * per, per), :, pl.ds(pl.multiple_of(c * BLK, BLK), BLK)],
            wdb.at[s, pl.ds(k * per, per)], dsem.at[s, k])

    own_h = pltpu.make_async_copy(h_hbm, hbuf.at[q_own], lsem.at[0])
    own_i = pltpu.make_async_copy(ids_hbm, idb.at[q_own], lsem.at[1])
    nw_c = pltpu.make_async_copy(nw_hbm, nwb, lsem.at[2])
    rw_c = pltpu.make_async_copy(rw_hbm, rwb, lsem.at[3])
    for cp in (own_h, own_i, nw_c, rw_c):
        cp.start()
    for e in range(RING):
        for cp in w_copies(e, e):
            cp.start()
    for c in range(2):
        for k in range(parts):
            d_copy(c, c, k).start()

    barrier = pltpu.get_barrier_semaphore()
    for dev in (partner, across, other):
        pl.semaphore_signal(barrier, inc=1, device_id=dev, device_id_type=MESH)
    pl.semaphore_wait(barrier, 3)

    def h_copy(src, q, dev, n):
        return pltpu.make_async_remote_copy(
            src_ref=src, dst_ref=hbuf.at[q], send_sem=hs_sem.at[n], recv_sem=hr_sem.at[n],
            device_id=dev, device_id_type=MESH)

    def i_copy(src, q, dev, n):
        return pltpu.make_async_remote_copy(
            src_ref=src, dst_ref=idb.at[q], send_sem=is_sem.at[n], recv_sem=ir_sem.at[n],
            device_id=dev, device_id_type=MESH)

    i_x = i_copy(ids_hbm, q_own, across, 0)
    i_p = i_copy(ids_hbm, q_own, partner, 1)
    h_x = h_copy(h_hbm, q_own, across, 0)
    h_p = h_copy(h_hbm, q_own, partner, 1)
    i_x.start()
    i_p.start()
    h_x.start()
    h_p.start()
    i_copy(ids_hbm, q_across, across, 0).wait_recv()
    i_r = i_copy(idb.at[q_across], q_across, partner, 2)
    i_r.start()

    own_i.wait()
    i_copy(ids_hbm, q_partner, partner, 1).wait_recv()
    i_copy(idb.at[q_diag], q_diag, partner, 2).wait_recv()
    ids_t = jnp.concatenate([idb[q] for q in range(4)], axis=1)
    exp_iota = lax.broadcasted_iota(jnp.int32, (n_exp, n_tok), 0)
    member = jnp.zeros((n_exp, n_tok), F32)
    for j in range(top_k):
        member = member + jnp.where(ids_t[j:j + 1, :] == exp_iota, 1.0, 0.0)
    row_i = lax.broadcasted_iota(jnp.int32, (n_tok, n_tok), 0)
    col_i = lax.broadcasted_iota(jnp.int32, (n_tok, n_tok), 1)
    before = jnp.where(row_i < col_i, 1.0, 0.0).astype(BF16)
    pos = jnp.dot(member.astype(BF16), before, preferred_element_type=F32)
    pos = jnp.where(member > 0.5, pos, -1.0)
    posb[...] = pos

    nw_c.wait()

    def norm_rows(q):
        wide = hbuf[q].astype(F32)
        inv = lax.rsqrt(jnp.mean(wide * wide, axis=-1, keepdims=True) + NORM_EPS)
        for k in range(d // 128):
            cols = pl.ds(k * 128, 128)
            part = hbuf[q, :, cols].astype(F32) * inv * nwb[k:k + 1, :].astype(F32)
            vbuf[pl.ds(pl.multiple_of(q * tok, tok), tok), cols] = part.astype(BF16)

    own_h.wait()
    norm_rows(q_own)
    h_copy(h_hbm, q_partner, partner, 1).wait_recv()
    norm_rows(q_partner)
    h_copy(h_hbm, q_across, across, 0).wait_recv()
    h_r = h_copy(hbuf.at[q_across], q_across, partner, 2)
    h_r.start()
    norm_rows(q_across)
    h_copy(hbuf.at[q_diag], q_diag, partner, 2).wait_recv()
    norm_rows(q_diag)

    pos_loc = posb[pl.ds(pl.multiple_of(ep * local, local), local), :]
    slot_f = lax.broadcasted_iota(jnp.int32, (slot_rows, n_tok), 0).astype(F32)
    pick = jnp.concatenate(
        [jnp.where(pos_loc[e:e + 1, :] == slot_f, 1.0, 0.0).astype(BF16) for e in range(local)], axis=0)

    def gather_cols(n, carry):
        cols = pl.ds(pl.multiple_of(n * 256, 256), 256)
        v_cols = vbuf[:, cols]
        for m in range(n_slots // 256):
            rows = jnp.dot(pick[m * 256:(m + 1) * 256], v_cols, preferred_element_type=F32)
            xbuf[m * 256:(m + 1) * 256, cols] = rows.astype(BF16)
        return carry

    lax.fori_loop(0, d // 256, gather_cols, 0)

    def gate_up(i, carry):
        first = i * UP_UNROLL
        for u in range(UP_UNROLL):
            for cp in w_copies(first + u, lax.rem(first + u, RING)):
                cp.wait()
        for u in range(UP_UNROLL):
            e = first + u
            rows = pl.ds(pl.multiple_of(e * slot_rows, slot_rows), slot_rows)
            pre = jnp.dot(xbuf[rows, :], ring[lax.rem(e, RING)], preferred_element_type=F32)
            gate, up = pre[:, :ff], pre[:, ff:]
            abuf[rows, :] = (gate * jax.nn.sigmoid(gate) * up).astype(BF16)

        @pl.when(first + RING < local)
        def _():
            for u in range(UP_UNROLL):
                for cp in w_copies(first + u + RING, lax.rem(first + u, RING)):
                    cp.start()
        return carry

    lax.fori_loop(0, local // UP_UNROLL, gate_up, 0)

    rw_c.wait()
    logits = jnp.dot(vbuf[...], rwb[...], preferred_element_type=F32)
    expo = jnp.exp(logits - jnp.max(logits, axis=-1, keepdims=True))
    prob = expo / jnp.sum(expo, axis=-1, keepdims=True)
    g_hi = prob.astype(BF16)
    rest = prob - g_hi.astype(F32)
    g_mid = rest.astype(BF16)
    g_lo = (rest - g_mid.astype(F32)).astype(BF16)
    pos_t = posb[...].T.astype(BF16)
    for n in range(n_slots // 256):
        lane = lax.broadcasted_iota(jnp.int32, (n_exp, 256), 1) + n * 256
        sub = lax.broadcasted_iota(jnp.int32, (n_exp, 256), 0)
        spread = jnp.where(sub == ep * local + lane // slot_rows, 1.0, 0.0).astype(BF16)
        want = (lax.broadcasted_iota(jnp.int32, (n_tok, 256), 1) % slot_rows).astype(F32)
        hit = jnp.dot(pos_t, spread, preferred_element_type=F32) == want
        for i, g in enumerate((g_hi, g_mid, g_lo)):
            wide_g = jnp.dot(g, spread, preferred_element_type=F32)
            cbuf[i, :, n * 256:(n + 1) * 256] = jnp.where(hit, wide_g, 0.0).astype(BF16)

    half = n_tok // 2

    def a_copy(c, row):
        return pltpu.make_async_remote_copy(
            src_ref=sbuf.at[c, pl.ds(pl.multiple_of(row * half, half), half)], dst_ref=ra.at[c],
            send_sem=as_sem.at[c], recv_sem=ar_sem.at[c], device_id=partner, device_id_type=MESH)

    def b_copy(c):
        return pltpu.make_async_remote_copy(
            src_ref=tb.at[c, pl.ds(pl.multiple_of((1 - x) * tok, tok), tok)], dst_ref=rb.at[c],
            send_sem=bs_sem.at[c], recv_sem=br_sem.at[c], device_id=across, device_id_type=MESH)

    def c_copy(c):
        return pltpu.make_async_remote_copy(
            src_ref=zb.at[c], dst_ref=rc.at[c],
            send_sem=cs_sem.at[c], recv_sem=cr_sem.at[c], device_id=other, device_id_type=MESH)

    def o_copy(c):
        cols = pl.ds(pl.multiple_of(c * BLK, BLK), BLK)
        return pltpu.make_async_copy(obuf.at[:, cols], out_hbm.at[:, cols], osem.at[c])

    def stage_b(c):
        a_copy(c, 1 - core).wait_recv()
        tb[c] = sbuf[c, pl.ds(pl.multiple_of(core * half, half), half), :] + ra[c]
        b_copy(c).start()

    def stage_c(c):
        b_copy(c).wait_recv()
        zb[c] = tb[c, pl.ds(pl.multiple_of(x * tok, tok), tok), :] + rb[c]
        c_copy(c).start()

    def stage_d(c):
        c_copy(c).wait_recv()
        cols = pl.ds(pl.multiple_of(c * BLK, BLK), BLK)
        obuf[:, cols] = (hbuf[q_own, :, cols].astype(F32) + (zb[c] + rc[c])).astype(BF16)
        o_copy(c).start()

    LAG_B, LAG_C, LAG_D = 1, 3, 5

    def down(c, carry):
        s = lax.rem(c, 2)
        for k in range(parts):
            d_copy(c, s, k).wait()

        def some(i, inner):
            for u in range(DOWN_UNROLL):
                e = i * DOWN_UNROLL + u
                rows = pl.ds(pl.multiple_of(e * slot_rows, slot_rows), slot_rows)
                y = jnp.dot(abuf[rows, :], wdb[s, e], preferred_element_type=F32)
                ybuf[rows, :] = y.astype(BF16)
            return inner

        lax.fori_loop(0, local // DOWN_UNROLL, some, 0)

        @pl.when(c + 2 < n_blk)
        def _():
            for k in range(parts):
                d_copy(c + 2, s, k).start()

        y_all = ybuf[...]
        total = jnp.dot(cbuf[2], y_all, preferred_element_type=F32)
        total = total + jnp.dot(cbuf[1], y_all, preferred_element_type=F32)
        total = total + jnp.dot(cbuf[0], y_all, preferred_element_type=F32)
        sbuf[c] = total
        a_copy(c, 1 - core).start()

        @pl.when(c >= LAG_B)
        def _():
            stage_b(c - LAG_B)

        @pl.when(c >= LAG_C)
        def _():
            stage_c(c - LAG_C)

        @pl.when(c >= LAG_D)
        def _():
            stage_d(c - LAG_D)
        return carry

    lax.fori_loop(0, n_blk, down, 0)
    for c in range(n_blk - LAG_B, n_blk):
        stage_b(c)
    for c in range(n_blk - LAG_C, n_blk):
        stage_c(c)
    for c in range(n_blk - LAG_D, n_blk):
        stage_d(c)

    for cp in (i_x, i_p, i_r, h_x, h_p, h_r):
        cp.wait_send()

    def drain(c, carry):
        a_copy(c, 1 - core).wait_send()
        b_copy(c).wait_send()
        c_copy(c).wait_send()
        o_copy(c).wait()
        return carry

    lax.fori_loop(0, n_blk, drain, 0)


def solution(mesh):
    def per_device(hidden, expert_ids, norm_w, router_w, w_gate, w_up, w_down):
        tok, d = hidden.shape
        top_k = expert_ids.shape[1]
        n_exp = router_w.shape[1]
        local, _, ff = w_gate.shape
        cap = row_cap(tok, top_k, n_exp)
        dims = (tok, top_k, n_exp, local, ff, d, cap)
        n_tok = 4 * tok
        n_slots = local * 4 * cap
        n_blk = d // BLK
        any_spec = pl.BlockSpec(memory_space=pl.ANY)
        dma = pltpu.SemaphoreType.DMA
        return pl.pallas_call(
            functools.partial(moe_kernel, dims),
            out_shape=jax.ShapeDtypeStruct((tok, d), BF16),
            in_specs=[any_spec] * 7,
            out_specs=any_spec,
            scratch_shapes=[
                pltpu.VMEM((RING, d, 2 * ff), BF16),
                pltpu.VMEM((2, local, ff, BLK), BF16),
                pltpu.VMEM((4, tok, d), BF16),
                pltpu.VMEM((4, top_k, tok), jnp.int32),
                pltpu.VMEM((d // 128, 128), BF16),
                pltpu.VMEM((d, n_exp), BF16),
                pltpu.VMEM((n_tok, d), BF16),
                pltpu.VMEM((n_slots, d), BF16),
                pltpu.VMEM((n_exp, n_tok), F32),
                pltpu.VMEM((3, n_tok, n_slots), BF16),
                pltpu.VMEM((n_slots, ff), BF16),
                pltpu.VMEM((n_slots, BLK), BF16),
                pltpu.VMEM((n_blk, n_tok, BLK), F32),
                pltpu.VMEM((n_blk, n_tok // 2, BLK), F32),
                pltpu.VMEM((n_blk, n_tok // 2, BLK), F32),
                pltpu.VMEM((n_blk, tok, BLK), F32),
                pltpu.VMEM((n_blk, tok, BLK), F32),
                pltpu.VMEM((n_blk, tok, BLK), F32),
                pltpu.VMEM((tok, d), BF16),
                dma((RING,)), dma((RING,)), dma((2, 4)), dma((4,)),
                dma((3,)), dma((3,)), dma((3,)), dma((3,)),
                dma((n_blk,)), dma((n_blk,)), dma((n_blk,)), dma((n_blk,)), dma((n_blk,)), dma((n_blk,)),
                dma((n_blk,)),
            ],
            compiler_params=pltpu.CompilerParams(
                collective_id=0, has_side_effects=True, vmem_limit_bytes=67043328),
            name="moe_layer",
        )(hidden, expert_ids.T, norm_w.reshape(d // 128, 128), router_w, w_gate, w_up, w_down)

    token_spec = P(("dp", "ep"), None)
    return jax.shard_map(per_device, mesh=mesh, in_specs=(token_spec, token_spec, P(None), P(None, None), P("ep", None, "tp"), P("ep", None, "tp"), P("ep", "tp", None)), out_specs=token_spec, check_vma=False)
```

```python
import functools

import jax
import jax.numpy as jnp
from jax import lax
from jax.experimental import pallas as pl
from jax.experimental.pallas import tpu as pltpu
from jax.sharding import PartitionSpec as P

NORM_EPS = 1e-6
POOL = 15
BLK = 256
UP_UNROLL = 2
LAG_B, LAG_C, LAG_D = 1, 3, 6
F32 = jnp.float32
BF16 = jnp.bfloat16


def row_cap(tok_dev, top_k, n_experts):
    return 8 * ((2 * top_k * tok_dev + 8 * n_experts - 1) // (8 * n_experts))


def moe_kernel(dims, h_hbm, ids_hbm, nw_hbm, rw_hbm, wg_hbm, wu_hbm, wd_hbm, out_hbm,
               pool, hbuf, idb, nwb, rwb, vbuf, xbuf, posb, cbuf, abuf, ybuf,
               sbuf, ra, tb, rb, zb, rc, obuf,
               wsem, lsem, hs_sem, hr_sem, is_sem, ir_sem,
               as_sem, ar_sem, bs_sem, br_sem, cs_sem, cr_sem, osem):
    tok, top_k, n_exp, local, ff, d, cap = dims
    n_tok = 4 * tok
    chip_tok = 2 * tok
    chip_rows = 2 * cap
    slot_rows = 4 * cap
    n_slots = local * slot_rows
    n_blk = d // BLK
    groups = 2 * ff // BLK
    per = groups * d // ff
    n_half = local // per
    n_chunks = local + n_blk * n_half
    ep = lax.axis_index("ep")
    x = ep // 2
    core = ep % 2
    partner = {"ep": x * 2 + (1 - core)}
    across = {"ep": (1 - x) * 2 + core}
    other = {"tp": 1 - lax.axis_index("tp")}
    MESH = pl.DeviceIdType.MESH
    q_own, q_partner = core, 1 - core
    q_across, q_diag = 2 + core, 3 - core

    def up_copies(e, slot):
        return [
            pltpu.make_async_copy(src.at[e], pool.at[slot, :, pl.ds(k * ff, ff)], wsem.at[slot, k])
            for k, src in enumerate((wg_hbm, wu_hbm))]

    def down_copies(j, slot):
        cols = pl.ds(pl.multiple_of((j // n_half) * BLK, BLK), BLK)
        first = (j % n_half) * per * ff
        return [
            pltpu.make_async_copy(
                wd_hbm.at[pl.ds(pl.multiple_of(first + g * d, d), d), cols],
                pool.at[slot, :, pl.ds(g * BLK, BLK)], wsem.at[slot, g])
            for g in range(groups)]

    def start_chunk(i):
        slot = lax.rem(i, POOL)

        @pl.when(i < local)
        def _():
            for cp in up_copies(i, slot):
                cp.start()

        @pl.when((i >= local) & (i < n_chunks))
        def _():
            for cp in down_copies(i - local, slot):
                cp.start()

    own_h = pltpu.make_async_copy(h_hbm, hbuf.at[q_own], lsem.at[0])
    own_i = pltpu.make_async_copy(ids_hbm, idb.at[q_own], lsem.at[1])
    nw_c = pltpu.make_async_copy(nw_hbm, nwb, lsem.at[2])
    rw_c = pltpu.make_async_copy(rw_hbm, rwb, lsem.at[3])
    own_h.start()
    own_i.start()
    nw_c.start()

    barrier = pltpu.get_barrier_semaphore()
    for dev in (partner, across, other):
        pl.semaphore_signal(barrier, inc=1, device_id=dev, device_id_type=MESH)

    def first_chunk(i, carry):
        for cp in up_copies(i, i):
            cp.start()
        return carry

    lax.fori_loop(0, POOL, first_chunk, 0)
    rw_c.start()
    own_h.wait()
    own_i.wait()
    pl.semaphore_wait(barrier, 3)

    def h_copy(q, dst, dev, n):
        return pltpu.make_async_remote_copy(
            src_ref=hbuf.at[q], dst_ref=hbuf.at[dst], send_sem=hs_sem.at[n], recv_sem=hr_sem.at[n],
            device_id=dev, device_id_type=MESH)

    def i_copy(q, dst, dev, n):
        return pltpu.make_async_remote_copy(
            src_ref=idb.at[q], dst_ref=idb.at[dst], send_sem=is_sem.at[n], recv_sem=ir_sem.at[n],
            device_id=dev, device_id_type=MESH)

    i_x = i_copy(q_own, q_across, across, 0)
    i_p = i_copy(q_own, q_own, partner, 1)
    i_r = i_copy(q_across, q_across, partner, 2)
    h_x = h_copy(q_own, q_across, across, 0)
    h_p = h_copy(q_own, q_own, partner, 1)
    h_r = h_copy(q_across, q_across, partner, 2)
    i_x.start()
    h_x.start()
    i_p.start()
    h_p.start()

    nw_c.wait()

    def norm_rows(q):
        wide = hbuf[q].astype(F32)
        inv = lax.rsqrt(jnp.mean(wide * wide, axis=-1, keepdims=True) + NORM_EPS)
        for k in range(d // 128):
            cols = pl.ds(k * 128, 128)
            part = hbuf[q, :, cols].astype(F32) * inv * nwb[k:k + 1, :].astype(F32)
            vbuf[pl.ds(pl.multiple_of(q * tok, tok), tok), cols] = part.astype(BF16)

    norm_rows(q_own)
    i_copy(q_partner, q_partner, partner, 1).wait_recv()
    i_x.wait_recv()
    i_r.start()
    i_copy(q_diag, q_diag, partner, 2).wait_recv()

    ids_t = jnp.concatenate([idb[q] for q in range(4)], axis=1)
    exp_iota = lax.broadcasted_iota(jnp.int32, (n_exp, n_tok), 0)
    member = jnp.zeros((n_exp, n_tok), F32)
    for j in range(top_k):
        member = member + jnp.where(ids_t[j:j + 1, :] == exp_iota, 1.0, 0.0)
    row_i = lax.broadcasted_iota(jnp.int32, (n_tok, n_tok), 0)
    col_i = lax.broadcasted_iota(jnp.int32, (n_tok, n_tok), 1)
    before = (row_i < col_i) & (row_i // chip_tok == col_i // chip_tok)
    pos = jnp.dot(member.astype(BF16), jnp.where(before, 1.0, 0.0).astype(BF16), preferred_element_type=F32)
    posb[...] = jnp.where(member > 0.5, pos, -1.0)

    h_copy(q_partner, q_partner, partner, 1).wait_recv()
    norm_rows(q_partner)

    pos_loc = posb[pl.ds(pl.multiple_of(ep * local, local), local), :]
    rank_f = lax.broadcasted_iota(jnp.int32, (chip_rows, chip_tok), 0).astype(F32)

    def gather_rows(chip):
        pos_chip = pos_loc[:, chip * chip_tok:(chip + 1) * chip_tok]
        pick = jnp.concatenate(
            [jnp.where(pos_chip[e:e + 1, :] == rank_f, 1.0, 0.0).astype(BF16) for e in range(local)], axis=0)

        def cols_step(n, carry):
            cols = pl.ds(pl.multiple_of(n * 256, 256), 256)
            v_cols = vbuf[chip * chip_tok:(chip + 1) * chip_tok, cols]
            rows = jnp.dot(pick, v_cols, preferred_element_type=F32).astype(BF16)
            xbuf[:, chip, :, cols] = rows.reshape(local, chip_rows, 256)
            return carry

        lax.fori_loop(0, d // 256, cols_step, 0)

    gather_rows(0)
    h_x.wait_recv()
    h_r.start()
    norm_rows(q_across)
    h_copy(q_diag, q_diag, partner, 2).wait_recv()
    norm_rows(q_diag)
    gather_rows(1)

    def gate_up(i, carry):
        first = i * UP_UNROLL
        for u in range(UP_UNROLL):
            for cp in up_copies(first + u, lax.rem(first + u, POOL)):
                cp.wait()
        for u in range(UP_UNROLL):
            e = first + u
            rows = pl.ds(pl.multiple_of(e * slot_rows, slot_rows), slot_rows)
            pre = jnp.dot(xbuf[e].reshape(slot_rows, d), pool[lax.rem(e, POOL)], preferred_element_type=F32)
            gate, up = pre[:, :ff], pre[:, ff:]
            abuf[rows, :] = (gate * jax.nn.sigmoid(gate) * up).astype(BF16)
        for u in range(UP_UNROLL):
            start_chunk(first + u + POOL)
        return carry

    trips = local // UP_UNROLL
    lax.fori_loop(0, trips // 2, gate_up, 0)

    rw_c.wait()
    logits = jnp.dot(vbuf[...], rwb[...], preferred_element_type=F32)
    expo = jnp.exp(logits - jnp.max(logits, axis=-1, keepdims=True))
    prob = expo / jnp.sum(expo, axis=-1, keepdims=True)
    g_hi = prob.astype(BF16)
    rest = prob - g_hi.astype(F32)
    g_mid = rest.astype(BF16)
    g_lo = (rest - g_mid.astype(F32)).astype(BF16)
    chip_of = lax.broadcasted_iota(jnp.int32, (n_exp, n_tok), 1) // chip_tok
    pos_all = posb[...]
    pos_all = jnp.where(pos_all < 0.0, -1.0, pos_all + (chip_of * chip_rows).astype(F32))
    pos_t = pos_all.T.astype(BF16)
    for n in range(n_slots // 256):
        lane = lax.broadcasted_iota(jnp.int32, (n_exp, 256), 1) + n * 256
        sub = lax.broadcasted_iota(jnp.int32, (n_exp, 256), 0)
        spread = jnp.where(sub == ep * local + lane // slot_rows, 1.0, 0.0).astype(BF16)
        want = (lax.broadcasted_iota(jnp.int32, (n_tok, 256), 1) % slot_rows).astype(F32)
        hit = jnp.dot(pos_t, spread, preferred_element_type=F32) == want
        for i, g in enumerate((g_hi, g_mid, g_lo)):
            wide_g = jnp.dot(g, spread, preferred_element_type=F32)
            cbuf[i, :, n * 256:(n + 1) * 256] = jnp.where(hit, wide_g, 0.0).astype(BF16)

    lax.fori_loop(trips // 2, trips, gate_up, 0)

    def a_copy(c):
        return pltpu.make_async_remote_copy(
            src_ref=sbuf.at[c, :, 1 - core], dst_ref=ra.at[c],
            send_sem=as_sem.at[c], recv_sem=ar_sem.at[c], device_id=partner, device_id_type=MESH)

    def b_copy(c):
        return pltpu.make_async_remote_copy(
            src_ref=tb.at[c, 1], dst_ref=rb.at[c],
            send_sem=bs_sem.at[c], recv_sem=br_sem.at[c], device_id=across, device_id_type=MESH)

    def c_copy(c):
        return pltpu.make_async_remote_copy(
            src_ref=zb.at[c], dst_ref=rc.at[c],
            send_sem=cs_sem.at[c], recv_sem=cr_sem.at[c], device_id=other, device_id_type=MESH)

    def o_copy(c):
        cols = pl.ds(pl.multiple_of(c * BLK, BLK), BLK)
        return pltpu.make_async_copy(obuf.at[:, cols], out_hbm.at[:, cols], osem.at[c])

    def stage_b(c):
        a_copy(c).wait_recv()
        tb[c] = sbuf[c, :, core] + ra[c]
        b_copy(c).start()

    def stage_c(c):
        b_copy(c).wait_recv()
        zb[c] = tb[c, 0] + rb[c]
        c_copy(c).start()

    def stage_d(c):
        c_copy(c).wait_recv()
        cols = pl.ds(pl.multiple_of(c * BLK, BLK), BLK)
        obuf[:, cols] = (hbuf[q_own, :, cols].astype(F32) + (zb[c] + rc[c])).astype(BF16)
        o_copy(c).start()

    def down(c, carry):
        for h in range(n_half):
            j = c * n_half + h
            slot = lax.rem(local + j, POOL)
            for cp in down_copies(j, slot):
                cp.wait()
            for k in range(per):
                e = h * per + k
                act = abuf[e * slot_rows:(e + 1) * slot_rows, :]
                first, last = k * ff, (k + 1) * ff
                y = None
                while first < last:
                    g, row = first // d, first % d
                    size = min(last - first, d - row)
                    lo = first - k * ff
                    part = jnp.dot(act[:, lo:lo + size], pool[slot, row:row + size, g * BLK:(g + 1) * BLK],
                                   preferred_element_type=F32)
                    y = part if y is None else y + part
                    first += size
                ybuf[k * slot_rows:(k + 1) * slot_rows, :] = y.astype(BF16)
            start_chunk(local + j + POOL)
            y_all = ybuf[...]
            slots = pl.ds(h * per * slot_rows, per * slot_rows)
            total = jnp.dot(cbuf[2, :, slots], y_all, preferred_element_type=F32)
            total = total + jnp.dot(cbuf[1, :, slots], y_all, preferred_element_type=F32)
            total = total + jnp.dot(cbuf[0, :, slots], y_all, preferred_element_type=F32)
            total = total.reshape(2, 2, tok, BLK)
            if h == 0:
                sbuf[c] = total
            else:
                sbuf[c] += total
        a_copy(c).start()

        for lag, stage in ((LAG_B, stage_b), (LAG_C, stage_c), (LAG_D, stage_d)):
            @pl.when(c >= lag)
            def _(lag=lag, stage=stage):
                stage(c - lag)
        return carry

    lax.fori_loop(0, n_blk, down, 0)
    for step in range(n_blk, n_blk + LAG_D):
        for lag, stage in ((LAG_B, stage_b), (LAG_C, stage_c), (LAG_D, stage_d)):
            if step - lag < n_blk:
                stage(step - lag)

    for cp in (i_x, i_p, i_r, h_x, h_p, h_r):
        cp.wait_send()

    def drain(c, carry):
        a_copy(c).wait_send()
        b_copy(c).wait_send()
        c_copy(c).wait_send()
        o_copy(c).wait()
        return carry

    lax.fori_loop(0, n_blk, drain, 0)


def solution(mesh):
    def per_device(hidden, expert_ids, norm_w, router_w, w_gate, w_up, w_down):
        tok, d = hidden.shape
        top_k = expert_ids.shape[1]
        n_exp = router_w.shape[1]
        local, _, ff = w_gate.shape
        cap = row_cap(tok, top_k, n_exp)
        dims = (tok, top_k, n_exp, local, ff, d, cap)
        n_tok = 4 * tok
        n_slots = local * 4 * cap
        n_blk = d // BLK
        groups = 2 * ff // BLK
        any_spec = pl.BlockSpec(memory_space=pl.ANY)
        dma = pltpu.SemaphoreType.DMA
        return pl.pallas_call(
            functools.partial(moe_kernel, dims),
            out_shape=jax.ShapeDtypeStruct((tok, d), BF16),
            in_specs=[any_spec] * 7,
            out_specs=any_spec,
            scratch_shapes=[
                pltpu.VMEM((POOL, d, 2 * ff), BF16),
                pltpu.VMEM((4, tok, d), BF16),
                pltpu.VMEM((4, top_k, tok), jnp.int32),
                pltpu.VMEM((d // 128, 128), BF16),
                pltpu.VMEM((d, n_exp), BF16),
                pltpu.VMEM((n_tok, d), BF16),
                pltpu.VMEM((local, 2, 2 * cap, d), BF16),
                pltpu.VMEM((n_exp, n_tok), F32),
                pltpu.VMEM((3, n_tok, n_slots), BF16),
                pltpu.VMEM((n_slots, ff), BF16),
                pltpu.VMEM((groups * d // ff * 4 * cap, BLK), BF16),
                pltpu.VMEM((n_blk, 2, 2, tok, BLK), F32),
                pltpu.VMEM((n_blk, 2, tok, BLK), F32),
                pltpu.VMEM((n_blk, 2, tok, BLK), F32),
                pltpu.VMEM((n_blk, tok, BLK), F32),
                pltpu.VMEM((n_blk, tok, BLK), F32),
                pltpu.VMEM((n_blk, tok, BLK), F32),
                pltpu.VMEM((tok, d), BF16),
                dma((POOL, groups)), dma((4,)),
                dma((3,)), dma((3,)), dma((3,)), dma((3,)),
                dma((n_blk,)), dma((n_blk,)), dma((n_blk,)), dma((n_blk,)), dma((n_blk,)), dma((n_blk,)),
                dma((n_blk,)),
            ],
            compiler_params=pltpu.CompilerParams(
                collective_id=0, has_side_effects=True, vmem_limit_bytes=67043328),
            name="moe_layer",
        )(hidden, expert_ids.T, norm_w.reshape(d // 128, 128), router_w, w_gate, w_up, w_down.reshape(local * ff, d))

    token_spec = P(("dp", "ep"), None)
    return jax.shard_map(per_device, mesh=mesh, in_specs=(token_spec, token_spec, P(None), P(None, None), P("ep", None, "tp"), P("ep", None, "tp"), P("ep", "tp", None)), out_specs=token_spec, check_vma=False)
```

```python
import functools

import jax
import jax.numpy as jnp
from jax import lax
from jax.experimental import pallas as pl
from jax.experimental.pallas import tpu as pltpu
from jax.sharding import PartitionSpec as P

NORM_EPS = 1e-6
POOL = 15
BLK = 256
LAST = 128
UP_UNROLL = 2
F32 = jnp.float32
BF16 = jnp.bfloat16


def row_cap(tok_dev, top_k, n_experts):
    return 8 * ((2 * top_k * tok_dev + 8 * n_experts - 1) // (8 * n_experts))


def moe_kernel(dims, h_hbm, ids_hbm, nw_hbm, rw_hbm, wg_hbm, wu_hbm, wd_hbm, out_ref,
               pool, hbuf, idb, nwb, rwb, vbuf, xbuf, posb, cbuf, abuf, ybuf,
               sbuf, ra, tb, rb, zb, rc, ylast, slast, ra2, tb2, r2,
               wsem, lsem, hs_sem, hr_sem, is_sem, ir_sem,
               as_sem, ar_sem, bs_sem, br_sem, cs_sem, cr_sem,
               as2_sem, ar2_sem, xs2_sem, xr2_sem):
    tok, top_k, n_exp, local, ff, d, cap = dims
    n_tok = 4 * tok
    chip_tok = 2 * tok
    chip_rows = 2 * cap
    slot_rows = 4 * cap
    n_slots = local * slot_rows
    n_big = d // BLK - 1
    groups = 2 * ff // BLK
    per = groups * d // ff
    n_half = local // per
    n_wide = local + n_big * n_half
    n_chunks = n_wide + BLK // LAST
    ep = lax.axis_index("ep")
    x = ep // 2
    core = ep % 2
    partner = {"ep": x * 2 + (1 - core)}
    across = {"ep": (1 - x) * 2 + core}
    other = {"tp": 1 - lax.axis_index("tp")}
    diag = {**other, **across}
    MESH = pl.DeviceIdType.MESH
    q_own, q_partner = core, 1 - core
    q_across, q_diag = 2 + core, 3 - core

    def up_copies(e, slot):
        return [
            pltpu.make_async_copy(src.at[e], pool.at[slot, :, pl.ds(k * ff, ff)], wsem.at[slot, k])
            for k, src in enumerate((wg_hbm, wu_hbm))]

    def down_copies(j, slot):
        cols = pl.ds(pl.multiple_of((j // n_half) * BLK, BLK), BLK)
        first = (j % n_half) * per * ff
        return [
            pltpu.make_async_copy(
                wd_hbm.at[pl.ds(pl.multiple_of(first + g * d, d), d), cols],
                pool.at[slot, :, pl.ds(g * BLK, BLK)], wsem.at[slot, g])
            for g in range(groups)]

    def last_copies(f, slot):
        cols = pl.ds(pl.multiple_of(n_big * BLK + f * LAST, LAST), LAST)
        return [
            pltpu.make_async_copy(
                wd_hbm.at[pl.ds(h * per * ff + g * d, d), cols],
                pool.at[slot, :, pl.ds(g * BLK + h * LAST, LAST)], wsem.at[slot, h * groups + g])
            for h in range(n_half) for g in range(groups)]

    def start_chunk(i):
        slot = lax.rem(i, POOL)

        @pl.when(i < local)
        def _():
            for cp in up_copies(i, slot):
                cp.start()

        @pl.when((i >= local) & (i < n_wide))
        def _():
            for cp in down_copies(i - local, slot):
                cp.start()

        @pl.when((i >= n_wide) & (i < n_chunks))
        def _():
            for cp in last_copies(i - n_wide, slot):
                cp.start()

    own_h = pltpu.make_async_copy(h_hbm, hbuf.at[q_own], lsem.at[0])
    own_i = pltpu.make_async_copy(ids_hbm, idb.at[q_own], lsem.at[1])
    nw_c = pltpu.make_async_copy(nw_hbm, nwb, lsem.at[2])
    rw_c = pltpu.make_async_copy(rw_hbm, rwb, lsem.at[3])
    own_h.start()
    own_i.start()
    nw_c.start()

    barrier = pltpu.get_barrier_semaphore()
    for dev in (partner, across, other, diag):
        pl.semaphore_signal(barrier, inc=1, device_id=dev, device_id_type=MESH)

    def first_chunk(i, carry):
        for cp in up_copies(i, i):
            cp.start()
        return carry

    lax.fori_loop(0, POOL, first_chunk, 0)
    rw_c.start()
    own_h.wait()
    own_i.wait()
    pl.semaphore_wait(barrier, 4)

    def h_copy(q, dst, dev, n):
        return pltpu.make_async_remote_copy(
            src_ref=hbuf.at[q], dst_ref=hbuf.at[dst], send_sem=hs_sem.at[n], recv_sem=hr_sem.at[n],
            device_id=dev, device_id_type=MESH)

    def i_copy(q, dst, dev, n):
        return pltpu.make_async_remote_copy(
            src_ref=idb.at[q], dst_ref=idb.at[dst], send_sem=is_sem.at[n], recv_sem=ir_sem.at[n],
            device_id=dev, device_id_type=MESH)

    i_x = i_copy(q_own, q_across, across, 0)
    i_p = i_copy(q_own, q_own, partner, 1)
    i_r = i_copy(q_across, q_across, partner, 2)
    h_x = h_copy(q_own, q_across, across, 0)
    h_p = h_copy(q_own, q_own, partner, 1)
    h_r = h_copy(q_across, q_across, partner, 2)
    i_x.start()
    h_x.start()
    i_p.start()
    h_p.start()

    nw_c.wait()

    def norm_rows(q):
        wide = hbuf[q].astype(F32)
        inv = lax.rsqrt(jnp.mean(wide * wide, axis=-1, keepdims=True) + NORM_EPS)
        for k in range(d // 128):
            cols = pl.ds(k * 128, 128)
            part = hbuf[q, :, cols].astype(F32) * inv * nwb[k:k + 1, :].astype(F32)
            vbuf[pl.ds(pl.multiple_of(q * tok, tok), tok), cols] = part.astype(BF16)

    norm_rows(q_own)
    i_copy(q_partner, q_partner, partner, 1).wait_recv()
    i_x.wait_recv()
    i_r.start()
    i_copy(q_diag, q_diag, partner, 2).wait_recv()

    ids_t = jnp.concatenate([idb[q] for q in range(4)], axis=1)
    exp_iota = lax.broadcasted_iota(jnp.int32, (n_exp, n_tok), 0)
    member = jnp.zeros((n_exp, n_tok), F32)
    for j in range(top_k):
        member = member + jnp.where(ids_t[j:j + 1, :] == exp_iota, 1.0, 0.0)
    row_i = lax.broadcasted_iota(jnp.int32, (n_tok, n_tok), 0)
    col_i = lax.broadcasted_iota(jnp.int32, (n_tok, n_tok), 1)
    before = (row_i < col_i) & (row_i // chip_tok == col_i // chip_tok)
    pos = jnp.dot(member.astype(BF16), jnp.where(before, 1.0, 0.0).astype(BF16), preferred_element_type=F32)
    posb[...] = jnp.where(member > 0.5, pos, -1.0)

    h_copy(q_partner, q_partner, partner, 1).wait_recv()
    norm_rows(q_partner)

    pos_loc = posb[pl.ds(pl.multiple_of(ep * local, local), local), :]
    rank_f = lax.broadcasted_iota(jnp.int32, (chip_rows, chip_tok), 0).astype(F32)

    def gather_rows(chip):
        pos_chip = pos_loc[:, chip * chip_tok:(chip + 1) * chip_tok]
        pick = jnp.concatenate(
            [jnp.where(pos_chip[e:e + 1, :] == rank_f, 1.0, 0.0).astype(BF16) for e in range(local)], axis=0)

        def cols_step(n, carry):
            cols = pl.ds(pl.multiple_of(n * 256, 256), 256)
            v_cols = vbuf[chip * chip_tok:(chip + 1) * chip_tok, cols]
            rows = jnp.dot(pick, v_cols, preferred_element_type=F32).astype(BF16)
            xbuf[:, chip, :, cols] = rows.reshape(local, chip_rows, 256)
            return carry

        lax.fori_loop(0, d // 256, cols_step, 0)

    gather_rows(0)
    h_x.wait_recv()
    h_r.start()
    norm_rows(q_across)
    h_copy(q_diag, q_diag, partner, 2).wait_recv()
    norm_rows(q_diag)
    gather_rows(1)

    def gate_up(i, carry):
        first = i * UP_UNROLL
        for u in range(UP_UNROLL):
            for cp in up_copies(first + u, lax.rem(first + u, POOL)):
                cp.wait()
        for u in range(UP_UNROLL):
            e = first + u
            rows = pl.ds(pl.multiple_of(e * slot_rows, slot_rows), slot_rows)
            pre = jnp.dot(xbuf[e].reshape(slot_rows, d), pool[lax.rem(e, POOL)], preferred_element_type=F32)
            gate, up = pre[:, :ff], pre[:, ff:]
            abuf[rows, :] = (gate * jax.nn.sigmoid(gate) * up).astype(BF16)
        for u in range(UP_UNROLL):
            start_chunk(first + u + POOL)
        return carry

    trips = local // UP_UNROLL
    lax.fori_loop(0, trips // 2, gate_up, 0)

    rw_c.wait()
    logits = jnp.dot(vbuf[...], rwb[...], preferred_element_type=F32)
    expo = jnp.exp(logits - jnp.max(logits, axis=-1, keepdims=True))
    prob = expo / jnp.sum(expo, axis=-1, keepdims=True)
    g_hi = prob.astype(BF16)
    rest = prob - g_hi.astype(F32)
    g_mid = rest.astype(BF16)
    g_lo = (rest - g_mid.astype(F32)).astype(BF16)
    chip_of = lax.broadcasted_iota(jnp.int32, (n_exp, n_tok), 1) // chip_tok
    pos_all = posb[...]
    pos_all = jnp.where(pos_all < 0.0, -1.0, pos_all + (chip_of * chip_rows).astype(F32))
    pos_t = pos_all.T.astype(BF16)
    for n in range(n_slots // 256):
        lane = lax.broadcasted_iota(jnp.int32, (n_exp, 256), 1) + n * 256
        sub = lax.broadcasted_iota(jnp.int32, (n_exp, 256), 0)
        spread = jnp.where(sub == ep * local + lane // slot_rows, 1.0, 0.0).astype(BF16)
        want = (lax.broadcasted_iota(jnp.int32, (n_tok, 256), 1) % slot_rows).astype(F32)
        hit = jnp.dot(pos_t, spread, preferred_element_type=F32) == want
        for i, g in enumerate((g_hi, g_mid, g_lo)):
            wide_g = jnp.dot(g, spread, preferred_element_type=F32)
            cbuf[i, :, n * 256:(n + 1) * 256] = jnp.where(hit, wide_g, 0.0).astype(BF16)

    lax.fori_loop(trips // 2, trips, gate_up, 0)

    def a_copy(c):
        return pltpu.make_async_remote_copy(
            src_ref=sbuf.at[c + 1, :, 1 - core], dst_ref=ra.at[c],
            send_sem=as_sem.at[c], recv_sem=ar_sem.at[c], device_id=partner, device_id_type=MESH)

    def b_copy(c):
        return pltpu.make_async_remote_copy(
            src_ref=tb.at[c, 1], dst_ref=rb.at[c],
            send_sem=bs_sem.at[c], recv_sem=br_sem.at[c], device_id=across, device_id_type=MESH)

    def c_copy(c):
        return pltpu.make_async_remote_copy(
            src_ref=zb.at[c], dst_ref=rc.at[c],
            send_sem=cs_sem.at[c], recv_sem=cr_sem.at[c], device_id=other, device_id_type=MESH)

    def stage_b(c):
        a_copy(c).wait_recv()
        tb[c] = sbuf[c + 1, :, core] + ra[c]
        b_copy(c).start()

    def stage_c(c):
        b_copy(c).wait_recv()
        zb[c] = tb[c, 0] + rb[c]
        c_copy(c).start()

    def stage_d(c):
        c_copy(c).wait_recv()
        cols = pl.ds(pl.multiple_of(c * BLK, BLK), BLK)
        out_ref[:, cols] = (hbuf[q_own, :, cols].astype(F32) + (zb[c] + rc[c])).astype(BF16)

    def a2_copy(f):
        return pltpu.make_async_remote_copy(
            src_ref=slast.at[f, :, 1 - core], dst_ref=ra2.at[f],
            send_sem=as2_sem.at[f], recv_sem=ar2_sem.at[f], device_id=partner, device_id_type=MESH)

    def x2_copies(f):
        return [
            pltpu.make_async_remote_copy(
                src_ref=tb2.at[f, src], dst_ref=r2.at[f, n],
                send_sem=xs2_sem.at[f, n], recv_sem=xr2_sem.at[f, n], device_id=dev, device_id_type=MESH)
            for n, (src, dev) in enumerate(((1, diag), (1, across), (0, other)))]

    def stage_x2(f):
        a2_copy(f).wait_recv()
        tb2[f] = slast[f, :, core] + ra2[f]
        for cp in x2_copies(f):
            cp.start()

    def stage_d2(f):
        for cp in x2_copies(f):
            cp.wait_recv()
        cols = pl.ds(n_big * BLK + f * LAST, LAST)
        moe = (tb2[f, 0] + r2[f, 1]) + (r2[f, 2] + r2[f, 0])
        out_ref[:, cols] = (hbuf[q_own, :, cols].astype(F32) + moe).astype(BF16)

    def act_rows(e):
        return abuf[e * slot_rows:(e + 1) * slot_rows, :]

    def split_k(k):
        first, last = k * ff, (k + 1) * ff
        while first < last:
            g, row = first // d, first % d
            size = min(last - first, d - row)
            yield g, row, size, first - k * ff
            first += size

    def down_half(slot, h):
        for k in range(per):
            act = act_rows(h * per + k)
            y = None
            for g, row, size, lo in split_k(k):
                part = jnp.dot(act[:, lo:lo + size], pool[slot, row:row + size, g * BLK:(g + 1) * BLK],
                               preferred_element_type=F32)
                y = part if y is None else y + part
            ybuf[h, k * slot_rows:(k + 1) * slot_rows, :] = y.astype(BF16)

    def down_last(slot):
        for k in range(per):
            act = jnp.concatenate([act_rows(h * per + k) for h in range(n_half)], axis=0)
            y = None
            for g, row, size, lo in split_k(k):
                part = jnp.dot(act[:, lo:lo + size], pool[slot, row:row + size, g * BLK:(g + 1) * BLK],
                               preferred_element_type=F32)
                y = part if y is None else y + part
            for h in range(n_half):
                e = h * per + k
                ylast[e * slot_rows:(e + 1) * slot_rows, :] = (
                    y[h * slot_rows:(h + 1) * slot_rows, h * LAST:(h + 1) * LAST].astype(BF16))

    def combine(y_all, slots):
        total = jnp.dot(cbuf[2, :, slots], y_all, preferred_element_type=F32)
        total = total + jnp.dot(cbuf[1, :, slots], y_all, preferred_element_type=F32)
        return total + jnp.dot(cbuf[0, :, slots], y_all, preferred_element_type=F32)

    half_slots = per * slot_rows

    def combine_half(h):
        return combine(ybuf[h], pl.ds(h * half_slots, half_slots)).reshape(2, 2, tok, BLK)

    def wait_down(j):
        slot = lax.rem(local + j, POOL)
        for cp in down_copies(j, slot):
            cp.wait()
        return slot

    def down(c, carry):
        slot = wait_down(2 * c)
        down_half(slot, 0)
        sbuf[c] += combine_half(1)
        start_chunk(local + 2 * c + POOL)

        @pl.when(c >= 1)
        def _():
            a_copy(c - 1).start()

        for lag, stage in ((2, stage_b), (4, stage_c), (6, stage_d)):
            @pl.when(c >= lag)
            def _(lag=lag, stage=stage):
                stage(c - lag)

        slot = wait_down(2 * c + 1)
        down_half(slot, 1)
        sbuf[c + 1] = combine_half(0)
        start_chunk(local + 2 * c + 1 + POOL)
        return carry

    lax.fori_loop(0, n_big, down, 0)

    all_slots = pl.ds(0, n_slots)
    slot = (n_chunks - 2) % POOL
    for cp in last_copies(0, slot):
        cp.wait()
    down_last(slot)
    sbuf[n_big] += combine_half(1)
    a_copy(n_big - 1).start()
    stage_b(n_big - 2)
    stage_c(n_big - 4)
    slast[0] = combine(ylast[...], all_slots).reshape(2, 2, tok, LAST)
    a2_copy(0).start()
    slot = (n_chunks - 1) % POOL
    for cp in last_copies(1, slot):
        cp.wait()
    down_last(slot)
    slast[1] = combine(ylast[...], all_slots).reshape(2, 2, tok, LAST)
    a2_copy(1).start()
    stage_b(n_big - 1)
    stage_c(n_big - 3)
    stage_x2(0)
    stage_x2(1)
    stage_d(n_big - 6)
    stage_c(n_big - 2)
    stage_d(n_big - 5)
    stage_d(n_big - 4)
    stage_c(n_big - 1)
    stage_d(n_big - 3)
    stage_d2(0)
    stage_d(n_big - 2)
    stage_d2(1)
    stage_d(n_big - 1)

    for cp in (i_x, i_p, i_r, h_x, h_p, h_r):
        cp.wait_send()

    def drain(c, carry):
        a_copy(c).wait_send()
        b_copy(c).wait_send()
        c_copy(c).wait_send()
        return carry

    lax.fori_loop(0, n_big, drain, 0)
    for f in range(2):
        a2_copy(f).wait_send()
        for cp in x2_copies(f):
            cp.wait_send()


def solution(mesh):
    def per_device(hidden, expert_ids, norm_w, router_w, w_gate, w_up, w_down):
        tok, d = hidden.shape
        top_k = expert_ids.shape[1]
        n_exp = router_w.shape[1]
        local, _, ff = w_gate.shape
        cap = row_cap(tok, top_k, n_exp)
        dims = (tok, top_k, n_exp, local, ff, d, cap)
        n_tok = 4 * tok
        n_slots = local * 4 * cap
        n_big = d // BLK - 1
        groups = 2 * ff // BLK
        any_spec = pl.BlockSpec(memory_space=pl.ANY)
        dma = pltpu.SemaphoreType.DMA
        return pl.pallas_call(
            functools.partial(moe_kernel, dims),
            out_shape=pltpu.VMEM((tok, d), BF16),
            in_specs=[any_spec] * 7,
            out_specs=pl.BlockSpec(memory_space=pltpu.VMEM),
            scratch_shapes=[
                pltpu.VMEM((POOL, d, 2 * ff), BF16),
                pltpu.VMEM((4, tok, d), BF16),
                pltpu.VMEM((4, top_k, tok), jnp.int32),
                pltpu.VMEM((d // 128, 128), BF16),
                pltpu.VMEM((d, n_exp), BF16),
                pltpu.VMEM((n_tok, d), BF16),
                pltpu.VMEM((local, 2, 2 * cap, d), BF16),
                pltpu.VMEM((n_exp, n_tok), F32),
                pltpu.VMEM((3, n_tok, n_slots), BF16),
                pltpu.VMEM((n_slots, ff), BF16),
                pltpu.VMEM((2, n_slots // 2, BLK), BF16),
                pltpu.VMEM((n_big + 1, 2, 2, tok, BLK), F32),
                pltpu.VMEM((n_big, 2, tok, BLK), F32),
                pltpu.VMEM((n_big, 2, tok, BLK), F32),
                pltpu.VMEM((n_big, tok, BLK), F32),
                pltpu.VMEM((n_big, tok, BLK), F32),
                pltpu.VMEM((n_big, tok, BLK), F32),
                pltpu.VMEM((n_slots, LAST), BF16),
                pltpu.VMEM((2, 2, 2, tok, LAST), F32),
                pltpu.VMEM((2, 2, tok, LAST), F32),
                pltpu.VMEM((2, 2, tok, LAST), F32),
                pltpu.VMEM((2, 3, tok, LAST), F32),
                dma((POOL, 2 * groups)), dma((4,)),
                dma((3,)), dma((3,)), dma((3,)), dma((3,)),
                dma((n_big,)), dma((n_big,)), dma((n_big,)), dma((n_big,)), dma((n_big,)), dma((n_big,)),
                dma((2,)), dma((2,)), dma((2, 3)), dma((2, 3)),
            ],
            compiler_params=pltpu.CompilerParams(
                collective_id=0, has_side_effects=True, vmem_limit_bytes=66500000),
            name="moe_layer",
        )(hidden, expert_ids.T, norm_w.reshape(d // 128, 128), router_w, w_gate, w_up, w_down.reshape(local * ff, d))

    token_spec = P(("dp", "ep"), None)
    return jax.shard_map(per_device, mesh=mesh, in_specs=(token_spec, token_spec, P(None), P(None, None), P("ep", None, "tp"), P("ep", None, "tp"), P("ep", "tp", None)), out_specs=token_spec, check_vma=False)
```

```python
import functools

import jax
import jax.numpy as jnp
from jax import lax
from jax.experimental import pallas as pl
from jax.experimental.pallas import tpu as pltpu
from jax.sharding import PartitionSpec as P

NORM_EPS = 1e-6
POOL = 15
BLK = 256
LAST = 128
UP_UNROLL = 2
SEEN = 6
F32 = jnp.float32
BF16 = jnp.bfloat16


def row_cap(tok_dev, top_k, n_experts):
    return 8 * ((2 * top_k * tok_dev + 8 * n_experts - 1) // (8 * n_experts))


def moe_kernel(dims, h_hbm, ids_hbm, nw_hbm, rw_hbm, wg_hbm, wu_hbm, wd_hbm, out_ref,
               pool, hbuf, idb, nwb, rwb, vbuf, xbuf, posb, cbuf, abuf, ybuf,
               sbuf, ra, tb, rb, zb, rc, ylast, slast, ra2, tb2, r2,
               wsem, lsem, hs_sem, hr_sem, is_sem, ir_sem,
               as_sem, ar_sem, bs_sem, br_sem, cs_sem, cr_sem,
               as2_sem, ar2_sem, xs2_sem, xr2_sem):
    tok, top_k, n_exp, local, ff, d, cap = dims
    n_tok = 4 * tok
    chip_tok = 2 * tok
    chip_rows = 2 * cap
    slot_rows = 4 * cap
    n_slots = local * slot_rows
    n_big = d // BLK - 1
    groups = 2 * ff // BLK
    per = groups * d // ff
    n_half = local // per
    n_wide = local + n_big * n_half
    n_chunks = n_wide + BLK // LAST
    ep = lax.axis_index("ep")
    x = ep // 2
    core = ep % 2
    partner = {"ep": x * 2 + (1 - core)}
    across = {"ep": (1 - x) * 2 + core}
    other = {"tp": 1 - lax.axis_index("tp")}
    diag = {**other, **across}
    MESH = pl.DeviceIdType.MESH
    q_own, q_partner = core, 1 - core
    q_across, q_diag = 2 + core, 3 - core

    def up_copies(e, slot):
        return [
            pltpu.make_async_copy(src.at[e], pool.at[slot, :, pl.ds(k * ff, ff)], wsem.at[slot, k])
            for k, src in enumerate((wg_hbm, wu_hbm))]

    def down_copies(j, slot):
        cols = pl.ds(pl.multiple_of((j // n_half) * BLK, BLK), BLK)
        first = (j % n_half) * per * ff
        return [
            pltpu.make_async_copy(
                wd_hbm.at[pl.ds(pl.multiple_of(first + g * d, d), d), cols],
                pool.at[slot, :, pl.ds(g * BLK, BLK)], wsem.at[slot, g])
            for g in range(groups)]

    def last_copies(f, slot):
        cols = pl.ds(pl.multiple_of(n_big * BLK + f * LAST, LAST), LAST)
        return [
            pltpu.make_async_copy(
                wd_hbm.at[pl.ds(h * per * ff + g * d, d), cols],
                pool.at[slot, :, pl.ds(g * BLK + h * LAST, LAST)], wsem.at[slot, h * groups + g])
            for h in range(n_half) for g in range(groups)]

    def start_chunk(i):
        slot = lax.rem(i, POOL)

        @pl.when(i < local)
        def _():
            for cp in up_copies(i, slot):
                cp.start()

        @pl.when((i >= local) & (i < n_wide))
        def _():
            for cp in down_copies(i - local, slot):
                cp.start()

        @pl.when((i >= n_wide) & (i < n_chunks))
        def _():
            for cp in last_copies(i - n_wide, slot):
                cp.start()

    own_h = pltpu.make_async_copy(h_hbm, hbuf.at[q_own], lsem.at[0])
    own_i = pltpu.make_async_copy(ids_hbm, idb.at[q_own], lsem.at[1])
    nw_c = pltpu.make_async_copy(nw_hbm, nwb, lsem.at[2])
    rw_c = pltpu.make_async_copy(rw_hbm, rwb, lsem.at[3])
    own_h.start()
    own_i.start()
    nw_c.start()

    barrier = pltpu.get_barrier_semaphore()
    for dev in (partner, across, other, diag):
        pl.semaphore_signal(barrier, inc=1, device_id=dev, device_id_type=MESH)

    def first_chunks(lo, hi):
        for i in range(lo, hi):
            for cp in up_copies(i, i):
                cp.start()

    def seen_chunks(lo, hi):
        for i in range(lo, hi):
            for cp in up_copies(i, i):
                cp.wait()

    first_chunks(0, 3)
    own_h.wait()
    own_i.wait()
    pl.semaphore_wait(barrier, 4)

    def h_copy(q, dst, dev, n):
        return pltpu.make_async_remote_copy(
            src_ref=hbuf.at[q], dst_ref=hbuf.at[dst], send_sem=hs_sem.at[n], recv_sem=hr_sem.at[n],
            device_id=dev, device_id_type=MESH)

    def i_copy(q, dst, dev, n):
        return pltpu.make_async_remote_copy(
            src_ref=idb.at[q], dst_ref=idb.at[dst], send_sem=is_sem.at[n], recv_sem=ir_sem.at[n],
            device_id=dev, device_id_type=MESH)

    i_x = i_copy(q_own, q_across, across, 0)
    i_p = i_copy(q_own, q_own, partner, 1)
    i_r = i_copy(q_across, q_across, partner, 2)
    h_x = h_copy(q_own, q_across, across, 0)
    h_p = h_copy(q_own, q_own, partner, 1)
    h_r = h_copy(q_across, q_across, partner, 2)
    i_x.start()
    h_x.start()
    i_p.start()
    h_p.start()
    first_chunks(3, 4)
    rw_c.start()

    nw_c.wait()

    def norm_rows(q):
        wide = hbuf[q].astype(F32)
        inv = lax.rsqrt(jnp.mean(wide * wide, axis=-1, keepdims=True) + NORM_EPS)
        for k in range(d // 128):
            cols = pl.ds(k * 128, 128)
            part = hbuf[q, :, cols].astype(F32) * inv * nwb[k:k + 1, :].astype(F32)
            vbuf[pl.ds(pl.multiple_of(q * tok, tok), tok), cols] = part.astype(BF16)

    norm_rows(q_own)
    seen_chunks(0, 1)
    first_chunks(4, 5)
    i_copy(q_partner, q_partner, partner, 1).wait_recv()
    i_x.wait_recv()
    i_r.start()
    seen_chunks(1, 3)
    first_chunks(5, 7)
    i_copy(q_diag, q_diag, partner, 2).wait_recv()

    ids_t = jnp.concatenate([idb[q] for q in range(4)], axis=1)
    exp_iota = lax.broadcasted_iota(jnp.int32, (n_exp, n_tok), 0)
    member = jnp.zeros((n_exp, n_tok), F32)
    for j in range(top_k):
        member = member + jnp.where(ids_t[j:j + 1, :] == exp_iota, 1.0, 0.0)
    row_i = lax.broadcasted_iota(jnp.int32, (n_tok, n_tok), 0)
    col_i = lax.broadcasted_iota(jnp.int32, (n_tok, n_tok), 1)
    before = (row_i < col_i) & (row_i // chip_tok == col_i // chip_tok)
    pos = jnp.dot(member.astype(BF16), jnp.where(before, 1.0, 0.0).astype(BF16), preferred_element_type=F32)
    posb[...] = jnp.where(member > 0.5, pos, -1.0)

    h_copy(q_partner, q_partner, partner, 1).wait_recv()
    norm_rows(q_partner)
    seen_chunks(3, 4)
    first_chunks(7, 8)

    pos_loc = posb[pl.ds(pl.multiple_of(ep * local, local), local), :]
    rank_f = lax.broadcasted_iota(jnp.int32, (chip_rows, chip_tok), 0).astype(F32)

    def gather_rows(chip):
        pos_chip = pos_loc[:, chip * chip_tok:(chip + 1) * chip_tok]
        pick = jnp.concatenate(
            [jnp.where(pos_chip[e:e + 1, :] == rank_f, 1.0, 0.0).astype(BF16) for e in range(local)], axis=0)

        def cols_step(i, carry):
            for u in range(4):
                cols = pl.ds(pl.multiple_of(i * 1024 + u * 256, 256), 256)
                v_cols = vbuf[chip * chip_tok:(chip + 1) * chip_tok, cols]
                rows = jnp.dot(pick, v_cols, preferred_element_type=F32).astype(BF16)
                xbuf[:, chip, :, cols] = rows.reshape(local, chip_rows, 256)
            return carry

        lax.fori_loop(0, d // 1024, cols_step, 0)

    gather_rows(0)
    seen_chunks(4, SEEN)
    first_chunks(8, 10)
    h_x.wait_recv()
    h_r.start()
    first_chunks(10, POOL)
    norm_rows(q_across)
    h_copy(q_diag, q_diag, partner, 2).wait_recv()
    norm_rows(q_diag)
    gather_rows(1)

    def gate_up(i, carry):
        first = i * UP_UNROLL
        @pl.when(first >= SEEN)
        def _():
            for u in range(UP_UNROLL):
                for cp in up_copies(first + u, lax.rem(first + u, POOL)):
                    cp.wait()

        for u in range(UP_UNROLL):
            e = first + u
            rows = pl.ds(pl.multiple_of(e * slot_rows, slot_rows), slot_rows)
            pre = jnp.dot(xbuf[e].reshape(slot_rows, d), pool[lax.rem(e, POOL)], preferred_element_type=F32)
            gate, up = pre[:, :ff], pre[:, ff:]
            abuf[rows, :] = (gate * jax.nn.sigmoid(gate) * up).astype(BF16)
        for u in range(UP_UNROLL):
            start_chunk(first + u + POOL)
        return carry

    trips = local // UP_UNROLL
    lax.fori_loop(0, trips // 2, gate_up, 0)

    rw_c.wait()
    logits = jnp.dot(vbuf[...], rwb[...], preferred_element_type=F32)
    expo = jnp.exp(logits - jnp.max(logits, axis=-1, keepdims=True))
    prob = expo / jnp.sum(expo, axis=-1, keepdims=True)
    g_hi = prob.astype(BF16)
    rest = prob - g_hi.astype(F32)
    g_mid = rest.astype(BF16)
    g_lo = (rest - g_mid.astype(F32)).astype(BF16)
    chip_of = lax.broadcasted_iota(jnp.int32, (n_exp, n_tok), 1) // chip_tok
    pos_all = posb[...]
    pos_all = jnp.where(pos_all < 0.0, -1.0, pos_all + (chip_of * chip_rows).astype(F32))
    pos_t = pos_all.T.astype(BF16)
    for n in range(n_slots // 256):
        lane = lax.broadcasted_iota(jnp.int32, (n_exp, 256), 1) + n * 256
        sub = lax.broadcasted_iota(jnp.int32, (n_exp, 256), 0)
        spread = jnp.where(sub == ep * local + lane // slot_rows, 1.0, 0.0).astype(BF16)
        want = (lax.broadcasted_iota(jnp.int32, (n_tok, 256), 1) % slot_rows).astype(F32)
        hit = jnp.dot(pos_t, spread, preferred_element_type=F32) == want
        for i, g in enumerate((g_hi, g_mid, g_lo)):
            wide_g = jnp.dot(g, spread, preferred_element_type=F32)
            cbuf[i, :, n * 256:(n + 1) * 256] = jnp.where(hit, wide_g, 0.0).astype(BF16)

    lax.fori_loop(trips // 2, trips, gate_up, 0)

    def a_copy(c):
        return pltpu.make_async_remote_copy(
            src_ref=sbuf.at[c + 1, :, 1 - core], dst_ref=ra.at[c],
            send_sem=as_sem.at[c], recv_sem=ar_sem.at[c], device_id=partner, device_id_type=MESH)

    def b_copy(c):
        return pltpu.make_async_remote_copy(
            src_ref=tb.at[c, 1], dst_ref=rb.at[c],
            send_sem=bs_sem.at[c], recv_sem=br_sem.at[c], device_id=across, device_id_type=MESH)

    def c_copy(c):
        return pltpu.make_async_remote_copy(
            src_ref=zb.at[c], dst_ref=rc.at[c],
            send_sem=cs_sem.at[c], recv_sem=cr_sem.at[c], device_id=other, device_id_type=MESH)

    def stage_b(c):
        a_copy(c).wait_recv()
        tb[c] = sbuf[c + 1, :, core] + ra[c]
        b_copy(c).start()

    def stage_c(c):
        b_copy(c).wait_recv()
        zb[c] = tb[c, 0] + rb[c]
        c_copy(c).start()

    def stage_d(c):
        c_copy(c).wait_recv()
        cols = pl.ds(pl.multiple_of(c * BLK, BLK), BLK)
        out_ref[:, cols] = (hbuf[q_own, :, cols].astype(F32) + (zb[c] + rc[c])).astype(BF16)

    def a2_copy(f):
        return pltpu.make_async_remote_copy(
            src_ref=slast.at[f, :, 1 - core], dst_ref=ra2.at[f],
            send_sem=as2_sem.at[f], recv_sem=ar2_sem.at[f], device_id=partner, device_id_type=MESH)

    def x2_copies(f):
        return [
            pltpu.make_async_remote_copy(
                src_ref=tb2.at[f, src], dst_ref=r2.at[f, n],
                send_sem=xs2_sem.at[f, n], recv_sem=xr2_sem.at[f, n], device_id=dev, device_id_type=MESH)
            for n, (src, dev) in enumerate(((1, diag), (1, across), (0, other)))]

    def stage_x2(f):
        a2_copy(f).wait_recv()
        tb2[f] = slast[f, :, core] + ra2[f]
        for cp in x2_copies(f):
            cp.start()

    def stage_d2(f):
        for cp in x2_copies(f):
            cp.wait_recv()
        cols = pl.ds(n_big * BLK + f * LAST, LAST)
        moe = (tb2[f, 0] + r2[f, 1]) + (r2[f, 2] + r2[f, 0])
        out_ref[:, cols] = (hbuf[q_own, :, cols].astype(F32) + moe).astype(BF16)

    def act_rows(e):
        return abuf[e * slot_rows:(e + 1) * slot_rows, :]

    def split_k(k):
        first, last = k * ff, (k + 1) * ff
        while first < last:
            g, row = first // d, first % d
            size = min(last - first, d - row)
            yield g, row, size, first - k * ff
            first += size

    def down_half(slot, h):
        for k in range(per):
            act = act_rows(h * per + k)
            y = None
            for g, row, size, lo in split_k(k):
                part = jnp.dot(act[:, lo:lo + size], pool[slot, row:row + size, g * BLK:(g + 1) * BLK],
                               preferred_element_type=F32)
                y = part if y is None else y + part
            ybuf[h, k * slot_rows:(k + 1) * slot_rows, :] = y.astype(BF16)

    def down_last(slot):
        for k in range(per):
            act = jnp.concatenate([act_rows(h * per + k) for h in range(n_half)], axis=0)
            y = None
            for g, row, size, lo in split_k(k):
                part = jnp.dot(act[:, lo:lo + size], pool[slot, row:row + size, g * BLK:(g + 1) * BLK],
                               preferred_element_type=F32)
                y = part if y is None else y + part
            for h in range(n_half):
                e = h * per + k
                ylast[e * slot_rows:(e + 1) * slot_rows, :] = (
                    y[h * slot_rows:(h + 1) * slot_rows, h * LAST:(h + 1) * LAST].astype(BF16))

    def combine(y_all, slots):
        total = jnp.dot(cbuf[2, :, slots], y_all, preferred_element_type=F32)
        total = total + jnp.dot(cbuf[1, :, slots], y_all, preferred_element_type=F32)
        return total + jnp.dot(cbuf[0, :, slots], y_all, preferred_element_type=F32)

    half_slots = per * slot_rows

    def combine_half(h):
        return combine(ybuf[h], pl.ds(h * half_slots, half_slots)).reshape(2, 2, tok, BLK)

    def wait_down(j):
        slot = lax.rem(local + j, POOL)
        for cp in down_copies(j, slot):
            cp.wait()
        return slot

    def down(c, carry):
        slot = wait_down(2 * c)
        down_half(slot, 0)
        sbuf[c] += combine_half(1)
        start_chunk(local + 2 * c + POOL)

        @pl.when(c >= 1)
        def _():
            a_copy(c - 1).start()

        for lag, stage in ((2, stage_b), (4, stage_c), (6, stage_d)):
            @pl.when(c >= lag)
            def _(lag=lag, stage=stage):
                stage(c - lag)

        slot = wait_down(2 * c + 1)
        down_half(slot, 1)
        sbuf[c + 1] = combine_half(0)
        start_chunk(local + 2 * c + 1 + POOL)
        return carry

    lax.fori_loop(0, n_big, down, 0)

    all_slots = pl.ds(0, n_slots)
    slot = (n_chunks - 2) % POOL
    for cp in last_copies(0, slot):
        cp.wait()
    down_last(slot)
    sbuf[n_big] += combine_half(1)
    a_copy(n_big - 1).start()
    stage_b(n_big - 2)
    stage_c(n_big - 4)
    slast[0] = combine(ylast[...], all_slots).reshape(2, 2, tok, LAST)
    a2_copy(0).start()
    slot = (n_chunks - 1) % POOL
    for cp in last_copies(1, slot):
        cp.wait()
    down_last(slot)
    slast[1] = combine(ylast[...], all_slots).reshape(2, 2, tok, LAST)
    a2_copy(1).start()
    stage_b(n_big - 1)
    stage_c(n_big - 3)
    stage_x2(0)
    stage_x2(1)
    stage_d(n_big - 6)
    stage_c(n_big - 2)
    stage_d(n_big - 5)
    stage_d(n_big - 4)
    stage_c(n_big - 1)
    stage_d(n_big - 3)
    stage_d2(0)
    stage_d(n_big - 2)
    stage_d2(1)
    stage_d(n_big - 1)

    for cp in (i_x, i_p, i_r, h_x, h_p, h_r):
        cp.wait_send()

    def drain(c, carry):
        a_copy(c).wait_send()
        b_copy(c).wait_send()
        c_copy(c).wait_send()
        return carry

    lax.fori_loop(0, n_big, drain, 0)
    for f in range(2):
        a2_copy(f).wait_send()
        for cp in x2_copies(f):
            cp.wait_send()


def solution(mesh):
    def per_device(hidden, expert_ids, norm_w, router_w, w_gate, w_up, w_down):
        tok, d = hidden.shape
        top_k = expert_ids.shape[1]
        n_exp = router_w.shape[1]
        local, _, ff = w_gate.shape
        cap = row_cap(tok, top_k, n_exp)
        dims = (tok, top_k, n_exp, local, ff, d, cap)
        n_tok = 4 * tok
        n_slots = local * 4 * cap
        n_big = d // BLK - 1
        groups = 2 * ff // BLK
        any_spec = pl.BlockSpec(memory_space=pl.ANY)
        dma = pltpu.SemaphoreType.DMA
        return pl.pallas_call(
            functools.partial(moe_kernel, dims),
            out_shape=pltpu.VMEM((tok, d), BF16),
            in_specs=[any_spec] * 7,
            out_specs=pl.BlockSpec(memory_space=pltpu.VMEM),
            scratch_shapes=[
                pltpu.VMEM((POOL, d, 2 * ff), BF16),
                pltpu.VMEM((4, tok, d), BF16),
                pltpu.VMEM((4, top_k, tok), jnp.int32),
                pltpu.VMEM((d // 128, 128), BF16),
                pltpu.VMEM((d, n_exp), BF16),
                pltpu.VMEM((n_tok, d), BF16),
                pltpu.VMEM((local, 2, 2 * cap, d), BF16),
                pltpu.VMEM((n_exp, n_tok), F32),
                pltpu.VMEM((3, n_tok, n_slots), BF16),
                pltpu.VMEM((n_slots, ff), BF16),
                pltpu.VMEM((2, n_slots // 2, BLK), BF16),
                pltpu.VMEM((n_big + 1, 2, 2, tok, BLK), F32),
                pltpu.VMEM((n_big, 2, tok, BLK), F32),
                pltpu.VMEM((n_big, 2, tok, BLK), F32),
                pltpu.VMEM((n_big, tok, BLK), F32),
                pltpu.VMEM((n_big, tok, BLK), F32),
                pltpu.VMEM((n_big, tok, BLK), F32),
                pltpu.VMEM((n_slots, LAST), BF16),
                pltpu.VMEM((2, 2, 2, tok, LAST), F32),
                pltpu.VMEM((2, 2, tok, LAST), F32),
                pltpu.VMEM((2, 2, tok, LAST), F32),
                pltpu.VMEM((2, 3, tok, LAST), F32),
                dma((POOL, 2 * groups)), dma((4,)),
                dma((3,)), dma((3,)), dma((3,)), dma((3,)),
                dma((n_big,)), dma((n_big,)), dma((n_big,)), dma((n_big,)), dma((n_big,)), dma((n_big,)),
                dma((2,)), dma((2,)), dma((2, 3)), dma((2, 3)),
            ],
            compiler_params=pltpu.CompilerParams(
                collective_id=0, has_side_effects=True, vmem_limit_bytes=66500000),
            name="moe_layer",
        )(hidden, expert_ids.T, norm_w.reshape(d // 128, 128), router_w, w_gate, w_up, w_down.reshape(local * ff, d))

    token_spec = P(("dp", "ep"), None)
    return jax.shard_map(per_device, mesh=mesh, in_specs=(token_spec, token_spec, P(None), P(None, None), P("ep", None, "tp"), P("ep", None, "tp"), P("ep", "tp", None)), out_specs=token_spec, check_vma=False)
```

```python
import functools

import jax
import jax.numpy as jnp
from jax import lax
from jax.experimental import pallas as pl
from jax.experimental.pallas import tpu as pltpu
from jax.sharding import PartitionSpec as P

NORM_EPS = 1e-6
POOL = 15
HALVED = 5
BLK = 256
LAST = 128
LANES = 128
UP_UNROLL = 2
F32 = jnp.float32
BF16 = jnp.bfloat16


def row_cap(tok_dev, top_k, n_experts):
    return 8 * ((2 * top_k * tok_dev + 8 * n_experts - 1) // (8 * n_experts))


def moe_kernel(dims, h_hbm, ids_hbm, nw_hbm, rw_hbm, wg_hbm, wu_hbm, wd_hbm, out_ref,
               pool, hbuf, idb, nwb, rwb, vbuf, xbuf, posb, cbuf, abuf, ybuf,
               sbuf, ra, tb, rb, zb, rc, ob, og, ylast, slast, ra2, tb2, z2, r2,
               wsem, lsem, hs_sem, hr_sem, is_sem, ir_sem,
               as_sem, ar_sem, bs_sem, br_sem, cs_sem, cr_sem,
               es_sem, er_sem, as2_sem, ar2_sem, xs2_sem, xr2_sem):
    tok, top_k, n_exp, local, ff, d, cap = dims
    n_tok = 4 * tok
    chip_tok = 2 * tok
    chip_rows = 2 * cap
    slot_rows = 4 * cap
    n_slots = local * slot_rows
    n_big = d // BLK - 1
    groups = 2 * ff // BLK
    per = groups * d // ff
    n_half = local // per
    n_wide = local + n_big * n_half
    n_chunks = n_wide + BLK // LAST
    ep = lax.axis_index("ep")
    x = ep // 2
    core = ep % 2
    partner = {"ep": x * 2 + (1 - core)}
    across = {"ep": (1 - x) * 2 + core}
    other = {"tp": 1 - lax.axis_index("tp")}
    tp = lax.axis_index("tp")
    MESH = pl.DeviceIdType.MESH
    q_own, q_partner = core, 1 - core
    q_across, q_diag = 2 + core, 3 - core

    def up_copies(e, slot):
        return [
            pltpu.make_async_copy(src.at[e], pool.at[slot, :, pl.ds(k * ff, ff)], wsem.at[slot, k])
            for k, src in enumerate((wg_hbm, wu_hbm))]

    def down_copies(j, slot):
        cols = pl.ds(pl.multiple_of((j // n_half) * BLK, BLK), BLK)
        first = (j % n_half) * per * ff
        return [
            pltpu.make_async_copy(
                wd_hbm.at[pl.ds(pl.multiple_of(first + g * d, d), d), cols],
                pool.at[slot, :, pl.ds(g * BLK, BLK)], wsem.at[slot, g])
            for g in range(groups)]

    def last_copies(f, slot):
        cols = pl.ds(pl.multiple_of(n_big * BLK + f * LAST, LAST), LAST)
        return [
            pltpu.make_async_copy(
                wd_hbm.at[pl.ds(h * per * ff + g * d, d), cols],
                pool.at[slot, :, pl.ds(g * BLK + h * LAST, LAST)], wsem.at[slot, h * groups + g])
            for h in range(n_half) for g in range(groups)]

    def start_chunk(i):
        slot = lax.rem(i, POOL)

        @pl.when(i < local)
        def _():
            for cp in up_copies(i, slot):
                cp.start()

        @pl.when((i >= local) & (i < n_wide))
        def _():
            for cp in down_copies(i - local, slot):
                cp.start()

        @pl.when((i >= n_wide) & (i < n_chunks))
        def _():
            for cp in last_copies(i - n_wide, slot):
                cp.start()

    own_h = pltpu.make_async_copy(h_hbm, hbuf.at[q_own], lsem.at[0])
    own_i = pltpu.make_async_copy(ids_hbm, idb.at[q_own], lsem.at[1])
    nw_c = pltpu.make_async_copy(nw_hbm, nwb, lsem.at[2])
    rw_c = pltpu.make_async_copy(rw_hbm, rwb, lsem.at[3])
    own_h.start()
    own_i.start()
    nw_c.start()
    rw_c.start()

    barrier = pltpu.get_barrier_semaphore()
    for dev in (partner, across, other):
        pl.semaphore_signal(barrier, inc=1, device_id=dev, device_id_type=MESH)

    for i in range(POOL):
        for cp in up_copies(i, i):
            cp.start()
    own_h.wait()
    own_i.wait()
    pl.semaphore_wait(barrier, 3)

    def h_copy(q, dst, dev, n):
        return pltpu.make_async_remote_copy(
            src_ref=hbuf.at[q], dst_ref=hbuf.at[dst], send_sem=hs_sem.at[n], recv_sem=hr_sem.at[n],
            device_id=dev, device_id_type=MESH)

    def i_copy(q, dst, dev, n):
        return pltpu.make_async_remote_copy(
            src_ref=idb.at[q], dst_ref=idb.at[dst], send_sem=is_sem.at[n], recv_sem=ir_sem.at[n],
            device_id=dev, device_id_type=MESH)

    i_x = i_copy(q_own, q_across, across, 0)
    i_p = i_copy(q_own, q_own, partner, 1)
    i_r = i_copy(q_across, q_across, partner, 2)
    h_x = h_copy(q_own, q_across, across, 0)
    h_p = h_copy(q_own, q_own, partner, 1)
    h_r = h_copy(q_across, q_across, partner, 2)
    i_x.start()
    h_x.start()
    i_p.start()
    h_p.start()

    nw_c.wait()

    def norm_rows(q):
        wide = hbuf[q].astype(F32)
        inv = lax.rsqrt(jnp.mean(wide * wide, axis=-1, keepdims=True) + NORM_EPS)
        for k in range(d // 128):
            cols = pl.ds(k * 128, 128)
            part = hbuf[q, :, cols].astype(F32) * inv * nwb[k:k + 1, :].astype(F32)
            vbuf[pl.ds(pl.multiple_of(q * tok, tok), tok), cols] = part.astype(BF16)

    norm_rows(q_own)
    i_copy(q_partner, q_partner, partner, 1).wait_recv()
    i_x.wait_recv()
    i_r.start()
    i_copy(q_diag, q_diag, partner, 2).wait_recv()

    ids_t = jnp.concatenate([idb[q] for q in range(4)], axis=1)
    exp_iota = lax.broadcasted_iota(jnp.int32, (n_exp, n_tok), 0)
    member = jnp.zeros((n_exp, n_tok), F32)
    for j in range(top_k):
        member = member + jnp.where(ids_t[j:j + 1, :] == exp_iota, 1.0, 0.0)
    row_i = lax.broadcasted_iota(jnp.int32, (n_tok, n_tok), 0)
    col_i = lax.broadcasted_iota(jnp.int32, (n_tok, n_tok), 1)
    before = (row_i < col_i) & (row_i // chip_tok == col_i // chip_tok)
    pos = jnp.dot(member.astype(BF16), jnp.where(before, 1.0, 0.0).astype(BF16), preferred_element_type=F32)
    posb[...] = jnp.where(member > 0.5, pos, -1.0)

    h_copy(q_partner, q_partner, partner, 1).wait_recv()
    norm_rows(q_partner)

    pos_loc = posb[pl.ds(pl.multiple_of(ep * local, local), local), :]
    rank_f = lax.broadcasted_iota(jnp.int32, (chip_rows, chip_tok), 0).astype(F32)

    def gather_rows(chip):
        pos_chip = pos_loc[:, chip * chip_tok:(chip + 1) * chip_tok]
        pick = jnp.concatenate(
            [jnp.where(pos_chip[e:e + 1, :] == rank_f, 1.0, 0.0).astype(BF16) for e in range(local)], axis=0)

        def cols_step(i, carry):
            for u in range(4):
                cols = pl.ds(pl.multiple_of(i * 1024 + u * 256, 256), 256)
                v_cols = vbuf[chip * chip_tok:(chip + 1) * chip_tok, cols]
                rows = jnp.dot(pick, v_cols, preferred_element_type=F32).astype(BF16)
                xbuf[:, chip, :, cols] = rows.reshape(local, chip_rows, 256)
            return carry

        lax.fori_loop(0, d // 1024, cols_step, 0)

    def router(chip):
        toks = slice(chip * chip_tok, (chip + 1) * chip_tok)
        logits = jnp.dot(vbuf[toks, :], rwb[...], preferred_element_type=F32)
        expo = jnp.exp(logits - jnp.max(logits, axis=-1, keepdims=True))
        prob = expo / jnp.sum(expo, axis=-1, keepdims=True)
        g_hi = prob.astype(BF16)
        rest = prob - g_hi.astype(F32)
        g_mid = rest.astype(BF16)
        g_lo = (rest - g_mid.astype(F32)).astype(BF16)
        pos_t = posb[:, toks].T.astype(BF16)
        n_cols = per * chip_rows
        for h in range(n_half):
            lane = lax.broadcasted_iota(jnp.int32, (n_exp, n_cols), 1)
            sub = lax.broadcasted_iota(jnp.int32, (n_exp, n_cols), 0)
            spread = jnp.where(sub == ep * local + h * per + lane // chip_rows, 1.0, 0.0).astype(BF16)
            want = (lax.broadcasted_iota(jnp.int32, (chip_tok, n_cols), 1) % chip_rows).astype(F32)
            hit = jnp.dot(pos_t, spread, preferred_element_type=F32) == want
            for i, g in enumerate((g_hi, g_mid, g_lo)):
                wide_g = jnp.dot(g, spread, preferred_element_type=F32)
                cbuf[h, chip, i * chip_tok:(i + 1) * chip_tok, :] = jnp.where(hit, wide_g, 0.0).astype(BF16)

    gather_rows(0)
    rw_c.wait()
    router(0)
    h_x.wait_recv()
    h_r.start()
    norm_rows(q_across)
    h_copy(q_diag, q_diag, partner, 2).wait_recv()
    norm_rows(q_diag)
    gather_rows(1)

    trips = local // UP_UNROLL

    def gate_up(i, carry):
        first = i * UP_UNROLL
        for u in range(UP_UNROLL):
            for cp in up_copies(first + u, lax.rem(first + u, POOL)):
                cp.wait()
        for u in range(UP_UNROLL):
            e = first + u
            rows = pl.ds(pl.multiple_of(e * slot_rows, slot_rows), slot_rows)
            pre = jnp.dot(xbuf[e].reshape(slot_rows, d), pool[lax.rem(e, POOL)], preferred_element_type=F32)
            gate, up = pre[:, :ff], pre[:, ff:]
            abuf[rows, :] = (gate * jax.nn.sigmoid(gate) * up).astype(BF16)
        for u in range(UP_UNROLL):
            start_chunk(first + u + POOL)

        @pl.when(i == trips // 2)
        def _():
            router(1)
        return carry

    lax.fori_loop(0, trips, gate_up, 0)


    def a_copy(c):
        return pltpu.make_async_remote_copy(
            src_ref=sbuf.at[c, :, 1 - core], dst_ref=ra.at[c],
            send_sem=as_sem.at[c], recv_sem=ar_sem.at[c], device_id=partner, device_id_type=MESH)

    def b_copy(c):
        return pltpu.make_async_remote_copy(
            src_ref=tb.at[c, 1], dst_ref=rb.at[c],
            send_sem=bs_sem.at[c], recv_sem=br_sem.at[c], device_id=across, device_id_type=MESH)

    def c_copy(c):
        return pltpu.make_async_remote_copy(
            src_ref=zb.at[c], dst_ref=rc.at[c],
            send_sem=cs_sem.at[c], recv_sem=cr_sem.at[c], device_id=other, device_id_type=MESH)

    def c_half_copy(c):
        return pltpu.make_async_remote_copy(
            src_ref=zb.at[c, 1 - tp], dst_ref=rc.at[c, 0],
            send_sem=cs_sem.at[c], recv_sem=cr_sem.at[c], device_id=other, device_id_type=MESH)

    def e_copy(c):
        return pltpu.make_async_remote_copy(
            src_ref=ob.at[c], dst_ref=og.at[c],
            send_sem=es_sem.at[c], recv_sem=er_sem.at[c], device_id=other, device_id_type=MESH)

    def stage_b(c):
        a_copy(c).wait_recv()
        tb[c] = sbuf[c, :, core] + ra[c]
        b_copy(c).start()

    def sum_x(c):
        b_copy(c).wait_recv()
        z = tb[c, 0] + rb[c]
        for n in range(2):
            zb[c, n] = z[:, n * LANES:(n + 1) * LANES]

    def stage_c_half(c):
        sum_x(c)
        c_half_copy(c).start()

    def stage_c(c):
        sum_x(c)
        c_copy(c).start()

    def half_cols(c, n):
        return pl.ds(pl.multiple_of(c * BLK + n * LANES, LANES), LANES)

    def stage_d_half(c):
        c_half_copy(c).wait_recv()
        ob[c] = (hbuf[q_own, :, half_cols(c, tp)].astype(F32) + (zb[c, tp] + rc[c, 0])).astype(BF16)
        e_copy(c).start()
        out_ref[:, half_cols(c, tp)] = ob[c]

    def stage_e(c):
        e_copy(c).wait_recv()
        out_ref[:, half_cols(c, 1 - tp)] = og[c]

    def stage_d(c):
        c_copy(c).wait_recv()
        for n in range(2):
            cols = half_cols(c, n)
            out_ref[:, cols] = (hbuf[q_own, :, cols].astype(F32) + (zb[c, n] + rc[c, n])).astype(BF16)

    def a2_copy(f):
        return pltpu.make_async_remote_copy(
            src_ref=slast.at[f, :, 1 - core], dst_ref=ra2.at[f],
            send_sem=as2_sem.at[f], recv_sem=ar2_sem.at[f], device_id=partner, device_id_type=MESH)

    def x2_copy(f):
        return pltpu.make_async_remote_copy(
            src_ref=tb2.at[f, 1], dst_ref=r2.at[f, 0],
            send_sem=xs2_sem.at[f, 0], recv_sem=xr2_sem.at[f, 0], device_id=across, device_id_type=MESH)

    def y2_copy(f):
        return pltpu.make_async_remote_copy(
            src_ref=z2.at[f], dst_ref=r2.at[f, 1],
            send_sem=xs2_sem.at[f, 1], recv_sem=xr2_sem.at[f, 1], device_id=other, device_id_type=MESH)

    def stage_b2(f):
        a2_copy(f).wait_recv()
        tb2[f] = slast[f, :, core] + ra2[f]
        x2_copy(f).start()

    def stage_c2(f):
        x2_copy(f).wait_recv()
        z2[f] = tb2[f, 0] + r2[f, 0]
        y2_copy(f).start()

    def stage_d2(f):
        y2_copy(f).wait_recv()
        cols = pl.ds(n_big * BLK + f * LAST, LAST)
        out_ref[:, cols] = (hbuf[q_own, :, cols].astype(F32) + (z2[f] + r2[f, 1])).astype(BF16)

    def act_rows(e):
        return abuf[e * slot_rows:(e + 1) * slot_rows, :]

    def split_k(k):
        first, last = k * ff, (k + 1) * ff
        while first < last:
            g, row = first // d, first % d
            size = min(last - first, d - row)
            yield g, row, size, first - k * ff
            first += size

    def down_half(slot, h):
        for k in range(per):
            act = act_rows(h * per + k)
            y = None
            for g, row, size, lo in split_k(k):
                part = jnp.dot(act[:, lo:lo + size], pool[slot, row:row + size, g * BLK:(g + 1) * BLK],
                               preferred_element_type=F32)
                y = part if y is None else y + part
            y = y.astype(BF16)
            for chip in range(2):
                ybuf[h, chip, k * chip_rows:(k + 1) * chip_rows, :] = y[chip * chip_rows:(chip + 1) * chip_rows]

    def down_last(slot):
        for k in range(per):
            act = jnp.concatenate([act_rows(h * per + k) for h in range(n_half)], axis=0)
            y = None
            for g, row, size, lo in split_k(k):
                part = jnp.dot(act[:, lo:lo + size], pool[slot, row:row + size, g * BLK:(g + 1) * BLK],
                               preferred_element_type=F32)
                y = part if y is None else y + part
            y = y.astype(BF16)
            for h in range(n_half):
                for chip in range(2):
                    row = h * slot_rows + chip * chip_rows
                    ylast[h, chip, k * chip_rows:(k + 1) * chip_rows, :] = y[row:row + chip_rows, h * LAST:(h + 1) * LAST]

    def combine(parts):
        sums = []
        for chip in range(2):
            lhs = jnp.concatenate([cbuf[h, chip] for h, _ in parts], axis=1)
            rhs = jnp.concatenate([y[h, chip] for h, y in parts], axis=0)
            wide = jnp.dot(lhs, rhs, preferred_element_type=F32)
            sums.append(wide[2 * chip_tok:] + wide[chip_tok:2 * chip_tok] + wide[:chip_tok])
        return jnp.stack(sums).reshape(2, 2, tok, -1)

    def combine_half(h):
        return combine([(h, ybuf)])

    def combine_last():
        return combine([(h, ylast) for h in range(n_half)])

    def wait_down(j):
        slot = lax.rem(local + j, POOL)
        for cp in down_copies(j, slot):
            cp.wait()
        return slot

    def down(c, carry):
        slot = wait_down(2 * c)
        down_half(slot, 0)

        @pl.when(c == 0)
        def _():
            start_chunk(local + POOL)

        @pl.when(c >= 4)
        def _():
            stage_c_half(c - 4)

        slot = wait_down(2 * c + 1)
        down_half(slot, 1)
        sbuf[c] = combine_half(0)
        sbuf[c] += combine_half(1)
        a_copy(c).start()

        @pl.when(c >= 1)
        def _():
            stage_b(c - 1)
        return carry

    lax.fori_loop(0, n_big, down, 0)

    def last_block(f):
        slot = (n_wide + f) % POOL
        for cp in last_copies(f, slot):
            cp.wait()
        down_last(slot)
        slast[f] = combine_last()
        a2_copy(f).start()

    last_block(0)
    stage_c_half(3)
    stage_b(6)
    stage_d_half(0)
    last_block(1)
    stage_b2(0)
    stage_c_half(4)
    stage_b2(1)
    stage_d_half(1)
    stage_c(5)
    stage_d_half(2)
    stage_c(6)
    stage_d_half(3)
    stage_c2(0)
    stage_c2(1)
    stage_d_half(4)
    for c in range(HALVED):
        stage_e(c)
    stage_d(5)
    stage_d(6)
    stage_d2(0)
    stage_d2(1)

    for cp in (i_x, i_p, i_r, h_x, h_p, h_r):
        cp.wait_send()

    for c in range(n_big):
        a_copy(c).wait_send()
        b_copy(c).wait_send()
        if c < HALVED:
            c_half_copy(c).wait_send()
            e_copy(c).wait_send()
        else:
            c_copy(c).wait_send()
    for f in range(2):
        a2_copy(f).wait_send()
        x2_copy(f).wait_send()
        y2_copy(f).wait_send()


def solution(mesh):
    def per_device(hidden, expert_ids, norm_w, router_w, w_gate, w_up, w_down):
        tok, d = hidden.shape
        top_k = expert_ids.shape[1]
        n_exp = router_w.shape[1]
        local, _, ff = w_gate.shape
        cap = row_cap(tok, top_k, n_exp)
        dims = (tok, top_k, n_exp, local, ff, d, cap)
        n_tok = 4 * tok
        n_slots = local * 4 * cap
        n_big = d // BLK - 1
        groups = 2 * ff // BLK
        any_spec = pl.BlockSpec(memory_space=pl.ANY)
        dma = pltpu.SemaphoreType.DMA
        return pl.pallas_call(
            functools.partial(moe_kernel, dims),
            out_shape=pltpu.VMEM((tok, d), BF16),
            in_specs=[any_spec] * 7,
            out_specs=pl.BlockSpec(memory_space=pltpu.VMEM),
            scratch_shapes=[
                pltpu.VMEM((POOL, d, 2 * ff), BF16),
                pltpu.VMEM((4, tok, d), BF16),
                pltpu.VMEM((4, top_k, tok), jnp.int32),
                pltpu.VMEM((d // 128, 128), BF16),
                pltpu.VMEM((d, n_exp), BF16),
                pltpu.VMEM((n_tok, d), BF16),
                pltpu.VMEM((local, 2, 2 * cap, d), BF16),
                pltpu.VMEM((n_exp, n_tok), F32),
                pltpu.VMEM((2, 2, 3 * n_tok // 2, n_slots // 4), BF16),
                pltpu.VMEM((n_slots, ff), BF16),
                pltpu.VMEM((2, 2, n_slots // 4, BLK), BF16),
                pltpu.VMEM((n_big, 2, 2, tok, BLK), F32),
                pltpu.VMEM((n_big, 2, tok, BLK), F32),
                pltpu.VMEM((n_big, 2, tok, BLK), F32),
                pltpu.VMEM((n_big, tok, BLK), F32),
                pltpu.VMEM((n_big, 2, tok, LANES), F32),
                pltpu.VMEM((n_big, 2, tok, LANES), F32),
                pltpu.VMEM((HALVED, tok, LANES), BF16),
                pltpu.VMEM((HALVED, tok, LANES), BF16),
                pltpu.VMEM((2, 2, n_slots // 4, LAST), BF16),
                pltpu.VMEM((2, 2, 2, tok, LAST), F32),
                pltpu.VMEM((2, 2, tok, LAST), F32),
                pltpu.VMEM((2, 2, tok, LAST), F32),
                pltpu.VMEM((2, tok, LAST), F32),
                pltpu.VMEM((2, 2, tok, LAST), F32),
                dma((POOL, 2 * groups)), dma((4,)),
                dma((3,)), dma((3,)), dma((3,)), dma((3,)),
                dma((n_big,)), dma((n_big,)), dma((n_big,)), dma((n_big,)), dma((n_big,)), dma((n_big,)),
                dma((HALVED,)), dma((HALVED,)), dma((2,)), dma((2,)), dma((2, 2)), dma((2, 2)),
            ],
            compiler_params=pltpu.CompilerParams(
                collective_id=0, has_side_effects=True, vmem_limit_bytes=66500000),
            name="moe_layer",
        )(hidden, expert_ids.T, norm_w.reshape(d // 128, 128), router_w, w_gate, w_up, w_down.reshape(local * ff, d))

    token_spec = P(("dp", "ep"), None)
    return jax.shard_map(per_device, mesh=mesh, in_specs=(token_spec, token_spec, P(None), P(None, None), P("ep", None, "tp"), P("ep", None, "tp"), P("ep", "tp", None)), out_specs=token_spec, check_vma=False)
```

```python
import functools

import jax
import jax.numpy as jnp
from jax import lax
from jax.experimental import pallas as pl
from jax.experimental.pallas import tpu as pltpu
from jax.sharding import PartitionSpec as P

NORM_EPS = 1e-6
POOL = 15
HALVED = 5
BLK = 256
LAST = 128
LANES = 128
UP_UNROLL = 2
F32 = jnp.float32
BF16 = jnp.bfloat16


def row_cap(tok_dev, top_k, n_experts):
    return 8 * ((2 * top_k * tok_dev + 8 * n_experts - 1) // (8 * n_experts))


def moe_kernel(dims, h_hbm, ids_hbm, nw_hbm, rw_hbm, wg_hbm, wu_hbm, wd_hbm, out_ref,
               pool, hbuf, idb, nwb, rwb, vbuf, xbuf, posb, cbuf, abuf, ybuf,
               sbuf, ra, tb, rb, zb, rc, ob, og, ylast, slast, ra2, tb2, z2, r2,
               wsem, lsem, hs_sem, hr_sem, is_sem, ir_sem,
               as_sem, ar_sem, bs_sem, br_sem, cs_sem, cr_sem,
               es_sem, er_sem, as2_sem, ar2_sem, xs2_sem, xr2_sem):
    tok, top_k, n_exp, local, ff, d, cap = dims
    n_tok = 4 * tok
    chip_tok = 2 * tok
    chip_rows = 2 * cap
    slot_rows = 4 * cap
    n_slots = local * slot_rows
    n_big = d // BLK - 1
    groups = 2 * ff // BLK
    per = groups * d // ff
    n_half = local // per
    n_wide = local + n_big * n_half
    n_chunks = n_wide + BLK // LAST
    ep = lax.axis_index("ep")
    x = ep // 2
    core = ep % 2
    partner = {"ep": x * 2 + (1 - core)}
    across = {"ep": (1 - x) * 2 + core}
    other = {"tp": 1 - lax.axis_index("tp")}
    tp = lax.axis_index("tp")
    MESH = pl.DeviceIdType.MESH
    q_own, q_partner = core, 1 - core
    q_across, q_diag = 2 + core, 3 - core

    def up_copies(e, slot):
        return [
            pltpu.make_async_copy(src.at[e], pool.at[slot, :, pl.ds(k * ff, ff)], wsem.at[slot, k])
            for k, src in enumerate((wg_hbm, wu_hbm))]

    def down_copies(j, slot):
        cols = pl.ds(pl.multiple_of((j // n_half) * BLK, BLK), BLK)
        first = (j % n_half) * per * ff
        return [
            pltpu.make_async_copy(
                wd_hbm.at[pl.ds(pl.multiple_of(first + g * d, d), d), cols],
                pool.at[slot, :, pl.ds(g * BLK, BLK)], wsem.at[slot, g])
            for g in range(groups)]

    def last_copies(f, slot):
        cols = pl.ds(pl.multiple_of(n_big * BLK + f * LAST, LAST), LAST)
        return [
            pltpu.make_async_copy(
                wd_hbm.at[pl.ds(h * per * ff + g * d, d), cols],
                pool.at[slot, :, pl.ds(g * BLK + h * LAST, LAST)], wsem.at[slot, h * groups + g])
            for h in range(n_half) for g in range(groups)]

    def start_chunk(i):
        slot = lax.rem(i, POOL)

        @pl.when(i < local)
        def _():
            for cp in up_copies(i, slot):
                cp.start()

        @pl.when((i >= local) & (i < n_wide))
        def _():
            for cp in down_copies(i - local, slot):
                cp.start()

        @pl.when((i >= n_wide) & (i < n_chunks))
        def _():
            for cp in last_copies(i - n_wide, slot):
                cp.start()

    own_h = pltpu.make_async_copy(h_hbm, hbuf.at[q_own], lsem.at[0])
    own_i = pltpu.make_async_copy(ids_hbm, idb.at[q_own], lsem.at[1])
    nw_c = pltpu.make_async_copy(nw_hbm, nwb, lsem.at[2])
    rw_c = pltpu.make_async_copy(rw_hbm, rwb, lsem.at[3])
    own_h.start()
    own_i.start()
    nw_c.start()
    rw_c.start()

    barrier = pltpu.get_barrier_semaphore()
    for dev in (partner, across, other):
        pl.semaphore_signal(barrier, inc=1, device_id=dev, device_id_type=MESH)

    for i in range(POOL):
        for cp in up_copies(i, i):
            cp.start()
    own_h.wait()
    own_i.wait()
    pl.semaphore_wait(barrier, 3)

    def h_copy(q, dst, dev, n):
        return pltpu.make_async_remote_copy(
            src_ref=hbuf.at[q], dst_ref=hbuf.at[dst], send_sem=hs_sem.at[n], recv_sem=hr_sem.at[n],
            device_id=dev, device_id_type=MESH)

    def i_copy(q, dst, dev, n):
        return pltpu.make_async_remote_copy(
            src_ref=idb.at[q], dst_ref=idb.at[dst], send_sem=is_sem.at[n], recv_sem=ir_sem.at[n],
            device_id=dev, device_id_type=MESH)

    i_x = i_copy(q_own, q_across, across, 0)
    i_p = i_copy(q_own, q_own, partner, 1)
    i_r = i_copy(q_across, q_across, partner, 2)
    h_x = h_copy(q_own, q_across, across, 0)
    h_p = h_copy(q_own, q_own, partner, 1)
    h_r = h_copy(q_across, q_across, partner, 2)
    i_x.start()
    h_x.start()
    i_p.start()
    h_p.start()

    nw_c.wait()

    def norm_rows(q):
        wide = hbuf[q].astype(F32)
        inv = lax.rsqrt(jnp.mean(wide * wide, axis=-1, keepdims=True) + NORM_EPS)
        for k in range(d // 128):
            cols = pl.ds(k * 128, 128)
            part = hbuf[q, :, cols].astype(F32) * inv * nwb[k:k + 1, :].astype(F32)
            vbuf[pl.ds(pl.multiple_of(q * tok, tok), tok), cols] = part.astype(BF16)

    norm_rows(q_own)
    i_copy(q_partner, q_partner, partner, 1).wait_recv()
    i_x.wait_recv()
    i_r.start()
    i_copy(q_diag, q_diag, partner, 2).wait_recv()

    ids_t = jnp.concatenate([idb[q] for q in range(4)], axis=1)
    exp_iota = lax.broadcasted_iota(jnp.int32, (n_exp, n_tok), 0)
    member = jnp.zeros((n_exp, n_tok), F32)
    for j in range(top_k):
        member = member + jnp.where(ids_t[j:j + 1, :] == exp_iota, 1.0, 0.0)
    row_i = lax.broadcasted_iota(jnp.int32, (n_tok, n_tok), 0)
    col_i = lax.broadcasted_iota(jnp.int32, (n_tok, n_tok), 1)
    before = (row_i < col_i) & (row_i // chip_tok == col_i // chip_tok)
    pos = jnp.dot(member.astype(BF16), jnp.where(before, 1.0, 0.0).astype(BF16), preferred_element_type=F32)
    posb[...] = jnp.where(member > 0.5, pos, -1.0)

    h_copy(q_partner, q_partner, partner, 1).wait_recv()
    norm_rows(q_partner)

    pos_loc = posb[pl.ds(pl.multiple_of(ep * local, local), local), :]
    rank_f = lax.broadcasted_iota(jnp.int32, (chip_rows, chip_tok), 0).astype(F32)

    def gather_rows(chip):
        pos_chip = pos_loc[:, chip * chip_tok:(chip + 1) * chip_tok]
        pick = jnp.concatenate(
            [jnp.where(pos_chip[e:e + 1, :] == rank_f, 1.0, 0.0).astype(BF16) for e in range(local)], axis=0)

        def cols_step(i, carry):
            for u in range(4):
                cols = pl.ds(pl.multiple_of(i * 1024 + u * 256, 256), 256)
                v_cols = vbuf[chip * chip_tok:(chip + 1) * chip_tok, cols]
                rows = jnp.dot(pick, v_cols, preferred_element_type=F32).astype(BF16)
                xbuf[:, chip, :, cols] = rows.reshape(local, chip_rows, 256)
            return carry

        lax.fori_loop(0, d // 1024, cols_step, 0)

    def router(chip):
        toks = slice(chip * chip_tok, (chip + 1) * chip_tok)
        logits = jnp.dot(vbuf[toks, :], rwb[...], preferred_element_type=F32)
        expo = jnp.exp(logits - jnp.max(logits, axis=-1, keepdims=True))
        prob = expo / jnp.sum(expo, axis=-1, keepdims=True)
        g_hi = prob.astype(BF16)
        rest = prob - g_hi.astype(F32)
        g_mid = rest.astype(BF16)
        g_lo = (rest - g_mid.astype(F32)).astype(BF16)
        pos_t = posb[:, toks].T.astype(BF16)
        n_cols = per * chip_rows
        for h in range(n_half):
            lane = lax.broadcasted_iota(jnp.int32, (n_exp, n_cols), 1)
            sub = lax.broadcasted_iota(jnp.int32, (n_exp, n_cols), 0)
            spread = jnp.where(sub == ep * local + h * per + lane // chip_rows, 1.0, 0.0).astype(BF16)
            want = (lax.broadcasted_iota(jnp.int32, (chip_tok, n_cols), 1) % chip_rows).astype(F32)
            hit = jnp.dot(pos_t, spread, preferred_element_type=F32) == want
            for i, g in enumerate((g_hi, g_mid, g_lo)):
                wide_g = jnp.dot(g, spread, preferred_element_type=F32)
                cbuf[h, chip, i * chip_tok:(i + 1) * chip_tok, :] = jnp.where(hit, wide_g, 0.0).astype(BF16)

    gather_rows(0)
    rw_c.wait()
    router(0)
    h_x.wait_recv()
    h_r.start()
    norm_rows(q_across)
    h_copy(q_diag, q_diag, partner, 2).wait_recv()
    norm_rows(q_diag)
    gather_rows(1)

    trips = local // UP_UNROLL

    def gate_up(i, carry):
        first = i * UP_UNROLL
        for u in range(UP_UNROLL):
            for cp in up_copies(first + u, lax.rem(first + u, POOL)):
                cp.wait()
        for u in range(UP_UNROLL):
            e = first + u
            rows = pl.ds(pl.multiple_of(e * slot_rows, slot_rows), slot_rows)
            pre = jnp.dot(xbuf[e].reshape(slot_rows, d), pool[lax.rem(e, POOL)], preferred_element_type=F32)
            gate, up = pre[:, :ff], pre[:, ff:]
            abuf[rows, :] = (gate * jax.nn.sigmoid(gate) * up).astype(BF16)
        for u in range(UP_UNROLL):
            start_chunk(first + u + POOL)

        @pl.when(i == trips // 2)
        def _():
            router(1)
        return carry

    lax.fori_loop(0, trips, gate_up, 0)


    def a_copy(c):
        return pltpu.make_async_remote_copy(
            src_ref=sbuf.at[c, :, 1 - core], dst_ref=ra.at[c],
            send_sem=as_sem.at[c], recv_sem=ar_sem.at[c], device_id=partner, device_id_type=MESH)

    def b_copy(c):
        return pltpu.make_async_remote_copy(
            src_ref=tb.at[c, 1], dst_ref=rb.at[c],
            send_sem=bs_sem.at[c], recv_sem=br_sem.at[c], device_id=across, device_id_type=MESH)

    def c_copy(c):
        return pltpu.make_async_remote_copy(
            src_ref=zb.at[c], dst_ref=rc.at[c],
            send_sem=cs_sem.at[c], recv_sem=cr_sem.at[c], device_id=other, device_id_type=MESH)

    def c_half_copy(c):
        return pltpu.make_async_remote_copy(
            src_ref=zb.at[c, 1 - tp], dst_ref=rc.at[c, 0],
            send_sem=cs_sem.at[c], recv_sem=cr_sem.at[c], device_id=other, device_id_type=MESH)

    def e_copy(c):
        return pltpu.make_async_remote_copy(
            src_ref=ob.at[c], dst_ref=og.at[c],
            send_sem=es_sem.at[c], recv_sem=er_sem.at[c], device_id=other, device_id_type=MESH)

    def stage_b(c):
        a_copy(c).wait_recv()
        tb[c] = sbuf[c, :, core] + ra[c]
        b_copy(c).start()

    def sum_x(c):
        b_copy(c).wait_recv()
        z = tb[c, 0] + rb[c]
        for n in range(2):
            zb[c, n] = z[:, n * LANES:(n + 1) * LANES]

    def stage_c_half(c):
        sum_x(c)
        c_half_copy(c).start()

    def stage_c(c):
        sum_x(c)
        c_copy(c).start()

    def half_cols(c, n):
        return pl.ds(pl.multiple_of(c * BLK + n * LANES, LANES), LANES)

    def stage_d_half(c):
        c_half_copy(c).wait_recv()
        ob[c] = (hbuf[q_own, :, half_cols(c, tp)].astype(F32) + (zb[c, tp] + rc[c, 0])).astype(BF16)
        e_copy(c).start()
        out_ref[:, half_cols(c, tp)] = ob[c]

    def stage_e(c):
        e_copy(c).wait_recv()
        out_ref[:, half_cols(c, 1 - tp)] = og[c]

    def stage_d(c):
        c_copy(c).wait_recv()
        for n in range(2):
            cols = half_cols(c, n)
            out_ref[:, cols] = (hbuf[q_own, :, cols].astype(F32) + (zb[c, n] + rc[c, n])).astype(BF16)

    def a2_copy(f):
        return pltpu.make_async_remote_copy(
            src_ref=slast.at[f, :, 1 - core], dst_ref=ra2.at[f],
            send_sem=as2_sem.at[f], recv_sem=ar2_sem.at[f], device_id=partner, device_id_type=MESH)

    def x2_copy(f):
        return pltpu.make_async_remote_copy(
            src_ref=tb2.at[f, 1], dst_ref=r2.at[f, 0],
            send_sem=xs2_sem.at[f, 0], recv_sem=xr2_sem.at[f, 0], device_id=across, device_id_type=MESH)

    def y2_copy(f):
        return pltpu.make_async_remote_copy(
            src_ref=z2.at[f], dst_ref=r2.at[f, 1],
            send_sem=xs2_sem.at[f, 1], recv_sem=xr2_sem.at[f, 1], device_id=other, device_id_type=MESH)

    def stage_b2(f):
        a2_copy(f).wait_recv()
        tb2[f] = slast[f, :, core] + ra2[f]
        x2_copy(f).start()

    def stage_c2(f):
        x2_copy(f).wait_recv()
        z2[f] = tb2[f, 0] + r2[f, 0]
        y2_copy(f).start()

    def stage_d2(f):
        y2_copy(f).wait_recv()
        cols = pl.ds(n_big * BLK + f * LAST, LAST)
        out_ref[:, cols] = (hbuf[q_own, :, cols].astype(F32) + (z2[f] + r2[f, 1])).astype(BF16)

    def act_rows(e):
        return abuf[e * slot_rows:(e + 1) * slot_rows, :]

    def split_k(k):
        first, last = k * ff, (k + 1) * ff
        while first < last:
            g, row = first // d, first % d
            size = min(last - first, d - row)
            yield g, row, size, first - k * ff
            first += size

    def down_half(slot, h):
        for k in range(per):
            act = act_rows(h * per + k)
            y = None
            for g, row, size, lo in split_k(k):
                part = jnp.dot(act[:, lo:lo + size], pool[slot, row:row + size, g * BLK:(g + 1) * BLK],
                               preferred_element_type=F32)
                y = part if y is None else y + part
            y = y.astype(BF16)
            for chip in range(2):
                ybuf[h, chip, k * chip_rows:(k + 1) * chip_rows, :] = y[chip * chip_rows:(chip + 1) * chip_rows]

    def down_last(slot):
        for k in range(per):
            act = jnp.concatenate([act_rows(h * per + k) for h in range(n_half)], axis=0)
            y = None
            for g, row, size, lo in split_k(k):
                part = jnp.dot(act[:, lo:lo + size], pool[slot, row:row + size, g * BLK:(g + 1) * BLK],
                               preferred_element_type=F32)
                y = part if y is None else y + part
            y = y.astype(BF16)
            for h in range(n_half):
                for chip in range(2):
                    row = h * slot_rows + chip * chip_rows
                    ylast[h, chip, k * chip_rows:(k + 1) * chip_rows, :] = y[row:row + chip_rows, h * LAST:(h + 1) * LAST]

    def combine(parts):
        sums = []
        for chip in range(2):
            lhs = jnp.concatenate([cbuf[h, chip] for h, _ in parts], axis=1)
            rhs = jnp.concatenate([y[h, chip] for h, y in parts], axis=0)
            wide = jnp.dot(lhs, rhs, preferred_element_type=F32)
            sums.append(wide[2 * chip_tok:] + wide[chip_tok:2 * chip_tok] + wide[:chip_tok])
        return jnp.stack(sums).reshape(2, 2, tok, -1)

    def combine_half(h):
        return combine([(h, ybuf)])

    def combine_last():
        return combine([(h, ylast) for h in range(n_half)])

    def wait_down(j):
        slot = lax.rem(local + j, POOL)
        for cp in down_copies(j, slot):
            cp.wait()
        return slot

    def down(c, carry):
        slot = wait_down(2 * c)
        down_half(slot, 0)

        @pl.when(c == 0)
        def _():
            start_chunk(local + POOL)

        @pl.when(c >= 2)
        def _():
            stage_b(c - 2)

        slot = wait_down(2 * c + 1)
        down_half(slot, 1)
        sbuf[c] = combine_half(0)
        sbuf[c] += combine_half(1)
        a_copy(c).start()

        @pl.when(c >= 4)
        def _():
            stage_c_half(c - 4)
        return carry

    lax.fori_loop(0, n_big, down, 0)

    def last_block(f):
        slot = (n_wide + f) % POOL
        for cp in last_copies(f, slot):
            cp.wait()
        down_last(slot)
        slast[f] = combine_last()
        a2_copy(f).start()

    last_block(0)
    stage_b(5)
    stage_b(6)
    stage_c_half(3)
    stage_d_half(0)
    last_block(1)
    stage_b2(0)
    stage_c_half(4)
    stage_b2(1)
    stage_d_half(1)
    stage_c(5)
    stage_d_half(2)
    stage_c(6)
    stage_d_half(3)
    stage_c2(0)
    stage_c2(1)
    stage_d_half(4)
    for c in range(HALVED):
        stage_e(c)
    stage_d(5)
    stage_d(6)
    stage_d2(0)
    stage_d2(1)

    for cp in (i_x, i_p, i_r, h_x, h_p, h_r):
        cp.wait_send()

    for c in range(n_big):
        a_copy(c).wait_send()
        b_copy(c).wait_send()
        if c < HALVED:
            c_half_copy(c).wait_send()
            e_copy(c).wait_send()
        else:
            c_copy(c).wait_send()
    for f in range(2):
        a2_copy(f).wait_send()
        x2_copy(f).wait_send()
        y2_copy(f).wait_send()


def solution(mesh):
    def per_device(hidden, expert_ids, norm_w, router_w, w_gate, w_up, w_down):
        tok, d = hidden.shape
        top_k = expert_ids.shape[1]
        n_exp = router_w.shape[1]
        local, _, ff = w_gate.shape
        cap = row_cap(tok, top_k, n_exp)
        dims = (tok, top_k, n_exp, local, ff, d, cap)
        n_tok = 4 * tok
        n_slots = local * 4 * cap
        n_big = d // BLK - 1
        groups = 2 * ff // BLK
        any_spec = pl.BlockSpec(memory_space=pl.ANY)
        dma = pltpu.SemaphoreType.DMA
        return pl.pallas_call(
            functools.partial(moe_kernel, dims),
            out_shape=pltpu.VMEM((tok, d), BF16),
            in_specs=[any_spec] * 7,
            out_specs=pl.BlockSpec(memory_space=pltpu.VMEM),
            scratch_shapes=[
                pltpu.VMEM((POOL, d, 2 * ff), BF16),
                pltpu.VMEM((4, tok, d), BF16),
                pltpu.VMEM((4, top_k, tok), jnp.int32),
                pltpu.VMEM((d // 128, 128), BF16),
                pltpu.VMEM((d, n_exp), BF16),
                pltpu.VMEM((n_tok, d), BF16),
                pltpu.VMEM((local, 2, 2 * cap, d), BF16),
                pltpu.VMEM((n_exp, n_tok), F32),
                pltpu.VMEM((2, 2, 3 * n_tok // 2, n_slots // 4), BF16),
                pltpu.VMEM((n_slots, ff), BF16),
                pltpu.VMEM((2, 2, n_slots // 4, BLK), BF16),
                pltpu.VMEM((n_big, 2, 2, tok, BLK), F32),
                pltpu.VMEM((n_big, 2, tok, BLK), F32),
                pltpu.VMEM((n_big, 2, tok, BLK), F32),
                pltpu.VMEM((n_big, tok, BLK), F32),
                pltpu.VMEM((n_big, 2, tok, LANES), F32),
                pltpu.VMEM((n_big, 2, tok, LANES), F32),
                pltpu.VMEM((HALVED, tok, LANES), BF16),
                pltpu.VMEM((HALVED, tok, LANES), BF16),
                pltpu.VMEM((2, 2, n_slots // 4, LAST), BF16),
                pltpu.VMEM((2, 2, 2, tok, LAST), F32),
                pltpu.VMEM((2, 2, tok, LAST), F32),
                pltpu.VMEM((2, 2, tok, LAST), F32),
                pltpu.VMEM((2, tok, LAST), F32),
                pltpu.VMEM((2, 2, tok, LAST), F32),
                dma((POOL, 2 * groups)), dma((4,)),
                dma((3,)), dma((3,)), dma((3,)), dma((3,)),
                dma((n_big,)), dma((n_big,)), dma((n_big,)), dma((n_big,)), dma((n_big,)), dma((n_big,)),
                dma((HALVED,)), dma((HALVED,)), dma((2,)), dma((2,)), dma((2, 2)), dma((2, 2)),
            ],
            compiler_params=pltpu.CompilerParams(
                collective_id=0, has_side_effects=True, vmem_limit_bytes=66500000),
            name="moe_layer",
        )(hidden, expert_ids.T, norm_w.reshape(d // 128, 128), router_w, w_gate, w_up, w_down.reshape(local * ff, d))

    token_spec = P(("dp", "ep"), None)
    return jax.shard_map(per_device, mesh=mesh, in_specs=(token_spec, token_spec, P(None), P(None, None), P("ep", None, "tp"), P("ep", None, "tp"), P("ep", "tp", None)), out_specs=token_spec, check_vma=False)
```
